256 devices in a mesh: gx: 16 (over z, core), gy: 16 (over x, y).
Axes of the slice: x: 4, y: 4, z: 8, core: 2. Of those that a mesh axis runs over, the one named last changes fastest.
Arguments:
- density: float32 [256, 256, 128], P('gx', 'gy'), may hold values from 0.05 to 40, as said below
Outputs:
- potential: float32 [256, 256, 128], P('gx', 'gy')
The draws below stay inside these ranges and needn't reach their ends.
Inputs may be any that keep to these rules, and one draw needn't show every extreme that they name: `density`: densities are positive.
All inputs are finite; a program needn't handle non-finite values.
Results may differ from the reference program's by a relative error of at most 0.00014.
Values sent between devices are 32-bit elements; how exact they have to be, the bound alone decides.
No kernel may reach another device: no remote copies, remote signals or barrier semaphores. Data moves between devices by JAX's collectives and lax.ppermute only.
A program may use at most 64 MiB of HBM per device.

```python
import jax
import jax.numpy as jnp

LEVELS = 4
NEWTON = 3
COARSE_SWEEPS = 2
NX = 256
NY = 256
NZ = 128


def draw_density(key, part):
    noise_key = jax.random.fold_in(jax.random.fold_in(key, 17), 0)
    noise_draw = jnp.clip(jax.random.normal(noise_key, (NX, NY, NZ), jnp.float32), -4.0, 4.0)
    coord_x = jnp.arange(NX, dtype=jnp.float32) / NX
    coord_y = jnp.arange(NY, dtype=jnp.float32) / NY
    tilt_factor = (1.0 + coord_x)[:, None, None] * (1.0 + coord_y)[None, :, None]
    density_field = jnp.exp(0.3 * noise_draw) * tilt_factor
    return density_field.astype(jnp.float32)


def setup_inputs(seed: int = 0) -> dict:
    key_of = jax.random.split(jax.random.key(seed), 2)
    return {
        "density": draw_density(jax.random.fold_in(key_of[1], 71), 0),
    }


COUPLING = 0.1
FLOOR = 3.0


def shifted(padded, off_x, off_y, off_z):
    size_x = padded.shape[0] - 2
    size_y = padded.shape[1] - 2
    size_z = padded.shape[2] - 2
    return padded[1 + off_x:1 + off_x + size_x, 1 + off_y:1 + off_y + size_y, 1 + off_z:1 + off_z + size_z]


def hessian(padded, spacing_inv):
    center = shifted(padded, 0, 0, 0)
    pure_x = (shifted(padded, 1, 0, 0) + shifted(padded, -1, 0, 0) - 2.0 * center) * spacing_inv
    pure_y = (shifted(padded, 0, 1, 0) + shifted(padded, 0, -1, 0) - 2.0 * center) * spacing_inv
    pure_z = (shifted(padded, 0, 0, 1) + shifted(padded, 0, 0, -1) - 2.0 * center) * spacing_inv
    quarter = 0.25 * spacing_inv
    mixed_xy = (shifted(padded, 1, 1, 0) - shifted(padded, 1, -1, 0) - shifted(padded, -1, 1, 0) + shifted(padded, -1, -1, 0)) * quarter
    mixed_xz = (shifted(padded, 1, 0, 1) - shifted(padded, 1, 0, -1) - shifted(padded, -1, 0, 1) + shifted(padded, -1, 0, -1)) * quarter
    mixed_yz = (shifted(padded, 0, 1, 1) - shifted(padded, 0, 1, -1) - shifted(padded, 0, -1, 1) + shifted(padded, 0, -1, -1)) * quarter
    return pure_x, pure_y, pure_z, mixed_xy, mixed_xz, mixed_yz


def nonlinear(padded, source):
    pure_x, pure_y, pure_z, mixed_xy, mixed_xz, mixed_yz = hessian(padded, 1.0)
    cubic = 2.0 * (pure_x * pure_y + pure_x * pure_z + pure_y * pure_z - mixed_xy * mixed_xy - mixed_xz * mixed_xz - mixed_yz * mixed_yz)
    return pure_x + pure_y + pure_z + COUPLING * cubic - source


def coefficients(padded, spacing_inv):
    pure_x, pure_y, pure_z, mixed_xy, mixed_xz, mixed_yz = hessian(padded, spacing_inv)
    stiff_x = 1.0 + 2.0 * COUPLING * (pure_y + pure_z)
    stiff_y = 1.0 + 2.0 * COUPLING * (pure_x + pure_z)
    stiff_z = 1.0 + 2.0 * COUPLING * (pure_x + pure_y)
    diagonal = jnp.maximum(2.0 * (stiff_x + stiff_y + stiff_z), FLOOR)
    relax = 1.0 / (spacing_inv * diagonal)
    return jnp.stack([stiff_x, stiff_y, stiff_z, -4.0 * COUPLING * mixed_xy, -4.0 * COUPLING * mixed_xz, -4.0 * COUPLING * mixed_yz, relax])


def jacobian(padded, weights, spacing_inv):
    parts = hessian(padded, spacing_inv)
    result = weights[0] * parts[0]
    for index in range(1, 6):
        result = result + weights[index] * parts[index]
    return result


def restrict(field):
    size_x, size_y, size_z = field.shape
    blocks = field.reshape(size_x // 2, 2, size_y // 2, 2, size_z // 2, 2)
    return jnp.sum(blocks, axis=(1, 3, 5)) * 0.125


def prolong(field):
    size_x, size_y, size_z = field.shape
    spread = jnp.broadcast_to(field[:, None, :, None, :, None], (size_x, 2, size_y, 2, size_z, 2))
    return spread.reshape(2 * size_x, 2 * size_y, 2 * size_z)


def wrap_all(field):
    return jnp.pad(field, 1, mode="wrap")


def checker(shape, first_x, first_y, first_z):
    index_x = first_x + jnp.arange(shape[0], dtype=jnp.int32)
    index_y = first_y + jnp.arange(shape[1], dtype=jnp.int32)
    index_z = first_z + jnp.arange(shape[2], dtype=jnp.int32)
    parity = (index_x[:, None, None] + index_y[None, :, None] + index_z[None, None, :]) % 2
    return (parity == 0).astype(jnp.float32)


def black_half(change, target, weights, red_mask, extend, spacing_inv):
    black_mask = 1.0 - red_mask
    return change + black_mask * (jacobian(extend(change), weights, spacing_inv) - target) * weights[6]


def first_sweep(target, weights, red_mask, extend, spacing_inv):
    change = -red_mask * target * weights[6]
    return black_half(change, target, weights, red_mask, extend, spacing_inv)


def full_sweep(change, target, weights, red_mask, extend, spacing_inv):
    change = change + red_mask * (jacobian(extend(change), weights, spacing_inv) - target) * weights[6]
    return black_half(change, target, weights, red_mask, extend, spacing_inv)


def cycle(coarse_level, target, weight_levels, mask_levels):
    spacing_inv = 0.25 ** coarse_level
    weights = weight_levels[coarse_level]
    red_mask = mask_levels[coarse_level]
    change = first_sweep(target, weights, red_mask, wrap_all, spacing_inv)
    if coarse_level == LEVELS - 1:
        for repeat in range(COARSE_SWEEPS - 1):
            change = full_sweep(change, target, weights, red_mask, wrap_all, spacing_inv)
        return change
    leftover = target - jacobian(wrap_all(change), weights, spacing_inv)
    change = change + prolong(cycle(coarse_level + 1, restrict(leftover), weight_levels, mask_levels))
    return full_sweep(change, target, weights, red_mask, wrap_all, spacing_inv)


def reference(density):
    source = density / (jnp.sum(density) / density.size) - 1.0
    potential = jnp.zeros_like(density)
    for newton_step in range(NEWTON):
        weight_levels = []
        mask_levels = []
        coarse = potential
        target = source
        for coarse_level in range(LEVELS):
            if coarse_level > 0:
                coarse = restrict(coarse)
            padded = wrap_all(coarse)
            if coarse_level == 0:
                target = -nonlinear(padded, source)
            weight_levels.append(coefficients(padded, 0.25 ** coarse_level))
            mask_levels.append(checker(coarse.shape, 0, 0, 0))
        potential = potential + cycle(0, target, weight_levels, mask_levels)
    return potential
```

```python
import functools

import jax
import jax.numpy as jnp
from jax import lax
from jax.experimental import pallas as pl
from jax.experimental.pallas import tpu as pltpu
from jax.sharding import PartitionSpec as P


INTERPRET = False
LANES = 128
BLOCK = 16
MARGINS = (12, 8, 4)
W1 = 24
W2 = 32
CHUNK = 8
VMEM = pltpu.MemorySpace.VMEM
SMEM = pltpu.MemorySpace.SMEM
UNROLL = {1: 8, 2: 4, 3: 2, 4: 2, 5: 1}


def roll(x, shift, axis):
    return pltpu.roll(x, shift % x.shape[axis], axis)


def iota(shape, axis):
    return lax.broadcasted_iota(jnp.int32, shape, axis)


def parity(rows, zs):
    shape = (rows, LANES)
    return (iota(shape, 0) + iota(shape, 1) // zs) & 1


def pures(v, i, zs):
    c, p, m = v[i], v[i + 1], v[i - 1]
    yp, ym = roll(c, -1, 0), roll(c, 1, 0)
    c2 = 2.0 * c
    xx = p + m - c2
    yy = yp + ym - c2
    zz = roll(c, -zs, 1) + roll(c, zs, 1) - c2
    return xx, yy, zz, p - m, yp - ym


def hessian(v, i, zs):
    xx, yy, zz, d, e = pures(v, i, zs)
    xy = roll(d, -1, 0) - roll(d, 1, 0)
    xz = roll(d, -zs, 1) - roll(d, zs, 1)
    yz = roll(e, -zs, 1) - roll(e, zs, 1)
    return xx, yy, zz, xy, xz, yz


def jacobian(v, i, zs, coef):
    if coef is None:
        xx, yy, zz, _, _ = pures(v, i, zs)
        return xx + yy + zz
    parts = hessian(v, i, zs)
    out = coef[0, i] * parts[0]
    for n in range(1, 6):
        out = out + coef[n, i] * parts[n]
    return out


def coef_of(coef, i, parts, s):
    xx, yy, zz, xy, xz, yz = parts
    g = 0.2 * s
    h = -0.025 * s
    rho = relax_of(xx, yy, zz, s)
    values = (1.0 + g * (yy + zz), 1.0 + g * (xx + zz), 1.0 + g * (xx + yy), h * xy, h * xz, h * yz, rho)
    return rho, [(coef, (n, i), value) for n, value in enumerate(values)]


def relax_of(xx, yy, zz, s):
    return 1.0 / jnp.maximum(6.0 + (0.8 * s) * (xx + yy + zz), 3.0)


def loop(lo, hi, f):
    def step(i, carry):
        f(i)
        return carry

    lax.fori_loop(lo, hi, step, 0)


def planes(lo, hi, rows, f):
    many = min(UNROLL[rows // 8], hi - lo)

    def group(first, count):
        done = [f(first + k) for k in range(count)]
        for stores in done:
            for ref, i, value in stores:
                ref[i] = value

    def step(g, carry):
        group(lo + g * many, many)
        return carry

    whole = (hi - lo) // many
    lax.fori_loop(0, whole, step, 0)
    if (hi - lo) % many:
        group(lo + whole * many, (hi - lo) % many)


def half(dst, src, t, coef, par, color, zs, lo, hi, ghosts=None):
    def f(i):
        c = src[i]
        rho = 1.0 / 6.0 if coef is None else coef[6, i]
        new = c + (jacobian(src, i, zs, coef) - t[i]) * rho
        return [(dst, i, jnp.where(par == ((i + color) & 1), new, c))]

    planes(lo, hi, par.shape[0], f)
    if ghosts:
        ghosts(dst)


def pair_z(s, zs):
    even = (iota(s.shape, 1) // zs) & 1 == 0
    return s + jnp.where(even, roll(s, -zs, 1), roll(s, zs, 1))


def restrict(plane, i, zs, rows, slot, row0, n):
    s = pair_z(plane(i) + plane(i + 1), zs)
    slot = jnp.int32(slot)
    rows[slot, pl.ds(0, s.shape[0]), :] = s
    return rows[slot, pl.ds(row0, n, stride=2), :] + rows[slot, pl.ds(row0 + 1, n, stride=2), :]


def double_rows(x, rows, slot):
    n = x.shape[0]
    slot = jnp.int32(slot)
    rows[slot, pl.ds(0, n, stride=2), :] = x
    rows[slot, pl.ds(1, n, stride=2), :] = x


def down0(m, inv, u, d, msg, v, t, coef, va, rows):
    w = BLOCK + 2 * m
    cut = MARGINS[0] - m
    flat = coef is None
    par = parity(w, 1)
    inv_m = inv[0, 0]

    def first(i):
        target = d[i + cut, cut : cut + w, :] * inv_m - 1.0
        stores = []
        if flat:
            rho = 1.0 / 6.0
        else:
            parts = hessian(u, i, 1)
            xx, yy, zz, xy, xz, yz = parts
            rho, stores = coef_of(coef, i, parts, 1.0)
            cubic = xx * yy + xx * zz + yy * zz - 0.0625 * (xy * xy + xz * xz + yz * yz)
            target = target - (xx + yy + zz) - 0.2 * cubic
        red = jnp.where(par == (i & 1), -target * rho, 0.0)
        return stores + [(t, i, target), (va, i, red)]

    edge = 0 if flat else 1
    planes(edge, w - edge, w, first)
    half(v, va, t, coef, par, 1, 1, edge + 1, w - edge - 1)
    lane_even = iota((8, LANES), 1) & 1 == 0

    def last(a):
        i = m + 2 * a
        t1 = 0.5 * restrict(lambda k: t[k] - jacobian(v, k, 1, coef), i, 1, rows, 2 * a, m, 8)
        if flat:
            u1 = jnp.zeros_like(t1)
        else:
            u1 = 0.125 * restrict(lambda k: u[k], i, 1, rows, 2 * a + 1, m, 8)
        return [(msg, a, jnp.where(lane_even, t1, u1))]

    planes(0, 8, 32, last)


def start(m, inv, db, do, da, msg, d, v, t, va, rows):
    n = BLOCK

    def load(a):
        d[a + m] = do[a]

    loop(0, n, load)

    def sides(a):
        d[a] = db[a]
        d[a + m + n] = da[a]

    loop(0, m, sides)
    down0(m, inv, None, d, msg, v, t, None, va, rows)


def down1(flat, *refs):
    if flat:
        wb, wo, wa, msg, lo, hi, v, t, va, rows = refs
        coef = None
    else:
        wb, wo, wa, msg, lo, hi, v, t, coef, va, u1, u2, rows = refs
    par = parity(W1, 2)
    even = iota((W1, LANES), 1) & 1 == 0

    def unpack(a):
        stores = []
        for k, w in enumerate((wb, wo, wa)):
            i = a + 8 * k
            p = w[a]
            target = jnp.where(even, p, roll(p, 1, 1))
            stores.append((t, i, target))
            if flat:
                stores.append((va, i, jnp.where(par == (i & 1), target * (-1.0 / 6.0), 0.0)))
            else:
                stores.append((u1, i, jnp.where(even, roll(p, -1, 1), p)))
        return stores

    planes(0, 8, 40, unpack)
    if not flat:

        def first(i):
            rho, stores = coef_of(coef, i, hessian(u1, i, 2), 0.25)
            return stores + [(va, i, jnp.where(par == (i & 1), -t[i] * rho, 0.0))]

        planes(1, W1 - 1, W1, first)

        def coarse(a):
            u = 0.125 * restrict(lambda k: u1[k], 2 * a, 2, rows, a, 0, 12)
            return [(u2, (a, slice(0, 12)), u)]

        planes(0, 12, W1, coarse)
    half(v, va, t, coef, par, 1, 2, 1 if flat else 3, W1 - (1 if flat else 3))
    phase = iota((8, LANES), 1) & 3
    par2 = parity(8, 4)

    def last(a):
        t2 = 0.5 * restrict(lambda k: t[k] - jacobian(v, k, 2, coef), 4 + 2 * a, 2, rows, 2 * a, 4, 8)
        if flat:
            red = jnp.where(par2 == (a & 1), t2 * (-1.0 / 6.0), 0.0)
            return [(msg, a, jnp.where(phase == 2, red, t2))]
        xx, yy, zz, _, _ = pures(u2, a + 2, 4)
        rho = relax_of(xx, yy, zz, 0.0625)
        rows[2 * a + 1, pl.ds(0, 16), :] = rho
        red = jnp.where(par2 == (a & 1), -t2 * rows[2 * a + 1, pl.ds(2, 8), :], 0.0)
        uc = u2[a + 2, 2:10, :]
        return [(msg, a, jnp.where(phase == 1, uc, jnp.where(phase == 2, red, t2)))]

    planes(0, 8, 32, last)
    lo[...] = msg[0:4]
    hi[...] = msg[4:8]


def repack(w0, w1, w2, w3, w4, out, lo, hi):
    phase = iota((8, LANES), 1) & 3
    where_from = [(w0, k) for k in range(4)]
    for w in (w1, w2, w3):
        where_from += [(w, k) for k in range(8)]
    where_from += [(w4, k) for k in range(4)]
    for a in range(CHUNK):
        for field in range(3):
            got = None
            for c in range(4):
                ref, k = where_from[a + CHUNK * c]
                part = ref[k]
                part = roll(part, c - field, 1) if c != field else part
                got = part if got is None else jnp.where(phase == c, part, got)
            out[field, a] = got
            lo[field, a] = got[0:4]
            hi[field, a] = got[4:8]


def ghosts_of(n):
    def fill(v):
        v[0] = roll(v[n], 1, 1)
        v[n + 1] = roll(v[1], -1, 1)

    return fill


def spread(x, c):
    phase = iota(x.shape, 1) & 3
    x = jnp.where(phase == c, x, 0.0)
    x = x + roll(x, -1 if c & 1 else 1, 1)
    return x + roll(x, -2 if c & 2 else 2, 1)


def up(m, flat, w2, s1, s0, u, out, scratch):
    v1, t1, c1 = s1
    v0, t0, c0 = s0
    u2, t2, va, vb, c2, u3, t3, e3, f3, c3, rows, v1b, v1c, v0b, v0c = scratch
    n2, n3 = CHUNK, CHUNK // 2
    g2, g3 = ghosts_of(n2), ghosts_of(n3)
    par2, par3 = parity(W2, 4), parity(W2 // 2, 8)

    def load(a):
        for field, ref in ((0, t2), (2, va)) + (() if flat else ((1, u2),)):
            row = 0
            for piece in w2:
                n = piece.shape[2]
                ref[a + 1, row : row + n, :] = piece[field, a]
                row += n

    for a in range(n2):
        load(a)
    g2(va)
    if flat:
        c2 = c3 = None
    else:
        g2(u2)
        planes(1, n2 + 1, W2, lambda i: coef_of(c2, i, hessian(u2, i, 4), 0.0625)[1])
    half(vb, va, t2, c2, par2, 0, 4, 1, n2 + 1, g2)

    def coarse(a):
        t = 0.5 * restrict(lambda k: t2[k] - jacobian(vb, k, 4, c2), 2 * a + 1, 4, rows, 2 * a, 0, 16)
        stores = [(t3, a + 1, t)]
        if not flat:
            x = 0.125 * restrict(lambda k: u2[k], 2 * a + 1, 4, rows, 2 * a + 1, 0, 16)
            stores.append((u3, a + 1, x))
        return stores

    planes(0, n3, 40, coarse)
    if not flat:
        g3(u3)

    def first(i):
        rho, stores = 1.0 / 6.0, []
        if not flat:
            rho, stores = coef_of(c3, i, hessian(u3, i, 8), 0.015625)
        return stores + [(e3, i, jnp.where(par3 == ((i + 1) & 1), -t3[i] * rho, 0.0))]

    planes(1, n3 + 1, W2 // 2, first)
    g3(e3)
    half(f3, e3, t3, c3, par3, 0, 8, 1, n3 + 1, g3)
    half(e3, f3, t3, c3, par3, 1, 8, 1, n3 + 1, g3)
    half(f3, e3, t3, c3, par3, 0, 8, 1, n3 + 1)

    for a in range(n3):
        double_rows(f3[a + 1], rows, a)
        e = rows[a, pl.ds(0, W2), :]
        va[2 * a + 1] = vb[2 * a + 1] + e
        va[2 * a + 2] = vb[2 * a + 2] + e
    g2(va)
    half(vb, va, t2, c2, par2, 1, 4, 1, n2 + 1, g2)
    half(va, vb, t2, c2, par2, 0, 4, 1, n2 + 1)

    for x in range(W1 // 2):
        k = x + 10
        double_rows(spread(va[(k & 7) + 1], k >> 3), rows, x)
        e = rows[x, pl.ds(20, W1), :]
        v1b[2 * x] = v1[2 * x] + e
        v1b[2 * x + 1] = v1[2 * x + 1] + e
    par1 = parity(W1, 2)
    r1 = m // 2
    half(v1c, v1b, t1, c1, par1, 0, 2, 8 - r1, 16 + r1)
    half(v1b, v1c, t1, c1, par1, 1, 2, 9 - r1, 15 + r1)

    w = BLOCK + 2 * m

    def raise0(a):
        double_rows(v1b[8 - m // 2 + a], rows, a)
        e = rows[a, pl.ds(16 - m, w), :]
        return [(v0b, 2 * a, v0[2 * a] + e), (v0b, 2 * a + 1, v0[2 * a + 1] + e)]

    planes(1, w // 2 - 1, w, raise0)
    par0 = parity(w, 1)
    half(v0c, v0b, t0, c0, par0, 0, 1, 3, w - 3)

    def final(a):
        i = a + 4
        c = v0c[i]
        rho = 1.0 / 6.0 if flat else c0[6, i]
        new = c + (jacobian(v0c, i, 1, c0) - t0[i]) * rho
        new = jnp.where(par0 == ((i + 1) & 1), new, c)
        if not flat:
            new = new + u[i]
        return [(out, a, new[4 : w - 4])]

    planes(0, w - 8, w, final)


def turn_end(m, has, *refs):
    flat, ends = has
    refs = list(refs)
    if not ends:
        inv, d = refs.pop(0), refs.pop(0)
    w2, refs = refs[:5], refs[5:]
    if flat:
        s1, s0, u, refs = [*refs[:2], None], [*refs[2:4], None], None, refs[4:]
    else:
        s1, s0, u, refs = refs[:3], refs[3:6], refs[6], refs[7:]
    out = refs.pop(0)
    if not ends:
        (msg, v, t, coef), refs = refs[:4], refs[4:]
    up(m, flat, w2, s1, s0, u, out, refs[:15])
    if not ends:
        down0(m - 4, inv, out, d, msg, v, t, coef, refs[15], refs[10])


def f32(*shape):
    return jax.ShapeDtypeStruct(shape, jnp.float32)


def scr(*shape):
    return pltpu.VMEM(shape, jnp.float32)


def call(body, name, outs, scratch, args, smem=0):
    specs = [pl.BlockSpec(memory_space=SMEM)] * smem
    specs += [pl.BlockSpec(memory_space=VMEM)] * (len(args) - smem)
    return pl.pallas_call(
        body,
        out_shape=outs,
        in_specs=specs,
        out_specs=[pl.BlockSpec(memory_space=VMEM)] * len(outs),
        scratch_shapes=scratch,
        interpret=INTERPRET,
        compiler_params=pltpu.CompilerParams(vmem_limit_bytes=16 << 20),
        name=name,
    )(*args)


def shift(x, axis, by):
    n = lax.axis_size(axis)
    return lax.ppermute(x, axis, [((i + by) % n, i) for i in range(n)])


def neighbours(x, axis, dim, width):
    n = x.shape[dim]
    before = shift(lax.slice_in_dim(x, n - width, n, axis=dim), axis, -1)
    after = shift(lax.slice_in_dim(x, 0, width, axis=dim), axis, 1)
    return before, x, after


def wide(x, lo, hi, axis):
    return shift(lo, axis, -3), shift(x, axis, -2), x, shift(x, axis, 2), shift(hi, axis, 3)


def total(x):
    for axis in ("gx", "gy"):
        n = lax.axis_size(axis)
        got = lax.all_to_all(jnp.broadcast_to(x, (n, 1, LANES)), axis, 0, 0)
        x = jnp.sum(got[:, 0, 0])
    return x


def per_device(density):
    cells = float(density.size * lax.axis_size("gx") * lax.axis_size("gy"))
    inv = jnp.reshape(cells / total(jnp.sum(density)), (1, 1))
    m = MARGINS[0]
    w = BLOCK + 2 * m
    d = jnp.concatenate(neighbours(density, "gy", 1, m), 1)
    rows = scr(24, 64, LANES)
    msg, d, *s0 = call(
        functools.partial(start, m),
        "start",
        [f32(8, 8, LANES)] + [f32(w, w, LANES)] * 3,
        [scr(w, w, LANES), rows],
        [inv, *neighbours(d, "gx", 0, m)],
        1,
    )
    u = []
    for turn, m in enumerate(MARGINS):
        flat, ends = turn == 0, turn == len(MARGINS) - 1
        w = BLOCK + 2 * m
        w1 = jnp.concatenate(neighbours(msg, "gy", 1, 8), 1)
        state = [f32(W1, W1, LANES)] * 2 + ([] if flat else [f32(7, W1, W1, LANES)])
        extra = [] if flat else [scr(W1, W1, LANES), scr(12, 16, LANES)]
        msg, lo, hi, *s1 = call(
            functools.partial(down1, flat),
            f"down1_{turn}",
            [f32(8, 8, LANES), f32(4, 8, LANES), f32(4, 8, LANES)] + state,
            [scr(W1, W1, LANES)] + extra + [rows],
            neighbours(w1, "gx", 0, 8),
        )
        packed = call(
            repack,
            f"repack_{turn}",
            [f32(3, 8, 8, LANES), f32(3, 8, 4, LANES), f32(3, 8, 4, LANES)],
            [],
            wide(msg, lo, hi, "gx"),
        )
        w2 = wide(*packed, "gy")
        a2 = scr(CHUNK + 2, W2, LANES)
        a3 = scr(CHUNK // 2 + 2, W2 // 2, LANES)
        scratch = [a2, a2, a2, a2, scr(7, CHUNK + 2, W2, LANES)]
        scratch += [a3, a3, a3, a3, scr(7, CHUNK // 2 + 2, W2 // 2, LANES)]
        scratch += [rows] + [scr(W1, W1, LANES)] * 2 + [scr(w, w, LANES)] * 2
        args = [*w2, *s1, *s0, *u]
        n = w - 8
        outs = [f32(n, n, LANES)]
        if not ends:
            args = [inv, d] + args
            outs += [f32(8, 8, LANES), f32(n, n, LANES), f32(n, n, LANES), f32(7, n, n, LANES)]
            scratch += [scr(n, n, LANES)]
        got = call(functools.partial(turn_end, m, (flat, ends)), f"up_{turn}", outs, scratch, args, int(not ends))
        if not ends:
            u, msg, *s0 = got
            u = [u]
    return got[0]


def solution(mesh):
    spec = P("gx", "gy", None)
    return jax.shard_map(per_device, mesh=mesh, in_specs=(spec,), out_specs=spec, check_vma=False)
```

```python
import functools

import jax
import jax.numpy as jnp
from jax import lax
from jax.experimental import pallas as pl
from jax.experimental.pallas import tpu as pltpu
from jax.sharding import PartitionSpec as P


INTERPRET = False
LANES = 128
BLOCK = 16
MARGINS = (12, 8, 4)
W1 = 24
W2 = 32
CHUNK = 8
VMEM = pltpu.MemorySpace.VMEM
SMEM = pltpu.MemorySpace.SMEM
UNROLL = {1: 8, 2: 4, 3: 12, 4: 16, 5: 12}


def roll(x, shift, axis):
    return pltpu.roll(x, shift % x.shape[axis], axis)


def iota(shape, axis):
    return lax.broadcasted_iota(jnp.int32, shape, axis)


def parity(rows, zs):
    shape = (rows, LANES)
    return (iota(shape, 0) + iota(shape, 1) // zs) & 1


def pures(v, i, zs):
    c, p, m = v[i], v[i + 1], v[i - 1]
    yp, ym = roll(c, -1, 0), roll(c, 1, 0)
    c2 = 2.0 * c
    xx = p + m - c2
    yy = yp + ym - c2
    zz = roll(c, -zs, 1) + roll(c, zs, 1) - c2
    return xx, yy, zz, p - m, yp - ym


def hessian(v, i, zs):
    xx, yy, zz, d, e = pures(v, i, zs)
    xy = roll(d, -1, 0) - roll(d, 1, 0)
    xz = roll(d, -zs, 1) - roll(d, zs, 1)
    yz = roll(e, -zs, 1) - roll(e, zs, 1)
    return xx, yy, zz, xy, xz, yz


def jacobian(v, i, zs, coef):
    if coef is None:
        xx, yy, zz, _, _ = pures(v, i, zs)
        return xx + yy + zz
    parts = hessian(v, i, zs)
    out = coef[0, i] * parts[0]
    for n in range(1, 6):
        out = out + coef[n, i] * parts[n]
    return out


def coef_of(coef, i, parts, s):
    xx, yy, zz, xy, xz, yz = parts
    g = 0.2 * s
    h = -0.025 * s
    rho = relax_of(xx, yy, zz, s)
    values = (1.0 + g * (yy + zz), 1.0 + g * (xx + zz), 1.0 + g * (xx + yy), h * xy, h * xz, h * yz, rho)
    return rho, [(coef, (n, i), value) for n, value in enumerate(values)]


def relax_of(xx, yy, zz, s):
    return 1.0 / jnp.maximum(6.0 + (0.8 * s) * (xx + yy + zz), 3.0)


def loop(lo, hi, f):
    def step(i, carry):
        f(i)
        return carry

    lax.fori_loop(lo, hi, step, 0)


def planes(lo, hi, rows, f):
    many = min(UNROLL[rows // 8], hi - lo)

    def group(first, count):
        done = [f(first + k) for k in range(count)]
        for stores in done:
            for ref, i, value in stores:
                ref[i] = value

    def step(g, carry):
        group(lo + g * many, many)
        return carry

    whole = (hi - lo) // many
    lax.fori_loop(0, whole, step, 0)
    if (hi - lo) % many:
        group(lo + whole * many, (hi - lo) % many)


def half(dst, src, t, coef, par, color, zs, lo, hi, ghosts=None, less=0.0):
    def f(i):
        c = src[i]
        rho = 1.0 / 6.0 if coef is None else coef[6, i]
        new = c + (jacobian(src, i, zs, coef) - (t[i] - less)) * rho
        return [(dst, i, jnp.where(par == ((i + color) & 1), new, c))]

    planes(lo, hi, par.shape[0], f)
    if ghosts:
        ghosts(dst)


def pair_z(s, zs):
    even = (iota(s.shape, 1) // zs) & 1 == 0
    return s + jnp.where(even, roll(s, -zs, 1), roll(s, zs, 1))


def restrict(plane, i, zs, rows, slot, row0, n):
    s = pair_z(plane(i) + plane(i + 1), zs)
    slot = jnp.int32(slot)
    rows[slot, pl.ds(0, s.shape[0]), :] = s
    return rows[slot, pl.ds(row0, n, stride=2), :] + rows[slot, pl.ds(row0 + 1, n, stride=2), :]


def double_rows(x, rows, slot):
    n = x.shape[0]
    slot = jnp.int32(slot)
    rows[slot, pl.ds(0, n, stride=2), :] = x
    rows[slot, pl.ds(1, n, stride=2), :] = x


def down0(m, inv, u, d, msg, v, t, coef, va, rows):
    w = BLOCK + 2 * m
    cut = MARGINS[0] - m
    flat = coef is None
    par = parity(w, 1)

    def first(i):
        if flat:
            return [(va, i, jnp.where(par == (i & 1), d[i] * (-1.0 / 6.0), 0.0))]
        target = d[i + cut, cut : cut + w, :] * inv[0:1, :] - 1.0
        parts = hessian(u, i, 1)
        xx, yy, zz, xy, xz, yz = parts
        rho, stores = coef_of(coef, i, parts, 1.0)
        cubic = xx * yy + xx * zz + yy * zz - 0.0625 * (xy * xy + xz * xz + yz * yz)
        target = target - (xx + yy + zz) - 0.2 * cubic
        red = jnp.where(par == (i & 1), -target * rho, 0.0)
        return stores + [(t, i, target), (va, i, red)]

    edge = 0 if flat else 1
    planes(edge, w - edge, w, first)
    half(v, va, t, coef, par, 1, 1, edge + 1, w - edge - 1)
    lane_even = iota((8, LANES), 1) & 1 == 0

    def last(a):
        i = m + 2 * a
        t1 = 0.5 * restrict(lambda k: t[k] - jacobian(v, k, 1, coef), i, 1, rows, 2 * a, m, 8)
        if flat:
            u1 = jnp.zeros_like(t1)
        else:
            u1 = 0.125 * restrict(lambda k: u[k], i, 1, rows, 2 * a + 1, m, 8)
        return [(msg, a, jnp.where(lane_even, t1, u1))]

    planes(0, 8, 32, last)


def merged(*tables):
    out = tables[0]
    for x in tables[1:]:
        out = jnp.maximum(out, x)
    return out


def pack_density(density, own, lo, hi):
    m = MARGINS[0]
    half_block = BLOCK // 2
    total = jnp.sum(jnp.sum(density[...], axis=0), keepdims=True)
    for k in range(BLOCK):
        p = k if k < half_block else k + 2
        x = density[k]
        own[p] = x
        lo[p] = x[0:m]
        hi[p] = x[BLOCK - m : BLOCK]
    row = iota((BLOCK, LANES), 0)
    lane = iota((BLOCK, LANES), 1)
    for k in range(2):
        here = (row + 8 * k == lax.axis_index("gx")) & (lane == lax.axis_index("gy")) & (row < 8)
        table = jnp.where(here, total, 0.0)
        own[half_block + k] = table
        lo[half_block + k] = table[0:m]
        hi[half_block + k] = table[0:m]


def start(m, db, do, da, msg, d, v, va, rows):
    half_block = BLOCK // 2
    for k in range(BLOCK):
        d[k + m] = do[k if k < half_block else k + 2]
    skip = BLOCK - m
    for k in range(m):
        d[k] = db[k if k + skip < half_block else k + 2]
        d[k + m + BLOCK] = da[k if k < half_block else k + 2]
    down0(m, None, None, d, msg, v, d, None, va, rows)
    for k in range(2):
        tables = []
        for ref, first in ((db, half_block - skip), (do, half_block), (da, half_block)):
            for row in (0, m, m + BLOCK):
                tables.append(ref[first + k, row : row + 8, :])
        msg[8 + k] = merged(*tables)


def down1(flat, *refs):
    if flat:
        wb, wo, wa, msg, lo, hi, known, v, t, va, rows = refs
        coef = None
    else:
        wb, wo, wa, msg, lo, hi, v, t, coef, va, u1, u2, rows = refs
    par = parity(W1, 2)
    even = iota((W1, LANES), 1) & 1 == 0

    def unpack(a):
        stores = []
        for k, w in enumerate((wb, wo, wa)):
            i = a + 8 * k
            p = w[a]
            target = jnp.where(even, p, roll(p, 1, 1))
            stores.append((t, i, target))
            if flat:
                stores.append((va, i, jnp.where(par == (i & 1), target * (-1.0 / 6.0), 0.0)))
            else:
                stores.append((u1, i, jnp.where(even, roll(p, -1, 1), p)))
        return stores

    planes(0, 8, 40, unpack)
    if not flat:

        def first(i):
            rho, stores = coef_of(coef, i, hessian(u1, i, 2), 0.25)
            return stores + [(va, i, jnp.where(par == (i & 1), -t[i] * rho, 0.0))]

        planes(1, W1 - 1, W1, first)

        def coarse(a):
            u = 0.125 * restrict(lambda k: u1[k], 2 * a, 2, rows, a, 0, 12)
            return [(u2, (a, slice(0, 12)), u)]

        planes(0, 12, W1, coarse)
    half(v, va, t, coef, par, 1, 2, 1 if flat else 3, W1 - (1 if flat else 3))
    phase = iota((8, LANES), 1) & 3
    par2 = parity(8, 4)

    def last(a):
        t2 = 0.5 * restrict(lambda k: t[k] - jacobian(v, k, 2, coef), 4 + 2 * a, 2, rows, 2 * a, 4, 8)
        if flat:
            red = jnp.where(par2 == (a & 1), t2 * (-1.0 / 6.0), 0.0)
            return [(msg, a, jnp.where(phase == 2, red, t2))]
        xx, yy, zz, _, _ = pures(u2, a + 2, 4)
        rho = relax_of(xx, yy, zz, 0.0625)
        rows[2 * a + 1, pl.ds(0, 16), :] = rho
        red = jnp.where(par2 == (a & 1), -t2 * rows[2 * a + 1, pl.ds(2, 8), :], 0.0)
        uc = u2[a + 2, 2:10, :]
        return [(msg, a, jnp.where(phase == 1, uc, jnp.where(phase == 2, red, t2)))]

    planes(0, 8, 32, last)
    lo[0:4] = msg[0:4]
    hi[0:4] = msg[4:8]
    if flat:
        for k in range(2):
            table = merged(*[w[8 + k, 8 * j : 8 * j + 8, :] for w in (wb, wo, wa) for j in range(3)])
            for ref in (msg, known):
                ref[ref.shape[0] - 2 + k] = table
            lo[4 + k] = table
            hi[4 + k] = table


def repack(flat, w0, w1, w2, w3, w4, *refs):
    if flat:
        far, out, lo, hi, known = refs
        for k in range(2):
            table = merged(*[w[w.shape[0] - 2 + k] for w in (w0, w1, w2, w3, w4, far)])
            known[k] = table
            out[1, k] = table
            for ref in (lo, hi):
                ref[1, 2 * k] = table[0:4]
                ref[1, 2 * k + 1] = table[4:8]
    else:
        out, lo, hi = refs
    phase = iota((8, LANES), 1) & 3
    where_from = [(w0, k) for k in range(4)]
    for w in (w1, w2, w3):
        where_from += [(w, k) for k in range(8)]
    where_from += [(w4, k) for k in range(4)]
    for a in range(CHUNK):
        for field in range(1 if flat else 3):
            got = None
            for c in range(4):
                ref, k = where_from[a + CHUNK * c]
                part = ref[k]
                part = roll(part, c - field, 1) if c != field else part
                got = part if got is None else jnp.where(phase == c, part, got)
            out[field, a] = got
            lo[field, a] = got[0:4]
            hi[field, a] = got[4:8]


def ghosts_of(n):
    def fill(v):
        v[0] = roll(v[n], 1, 1)
        v[n + 1] = roll(v[1], -1, 1)

    return fill


def spread(x, c):
    phase = iota(x.shape, 1) & 3
    x = jnp.where(phase == c, x, 0.0)
    x = x + roll(x, -1 if c & 1 else 1, 1)
    return x + roll(x, -2 if c & 2 else 2, 1)


def mean_of(w2, far, cells):
    total = None
    for k in range(2):
        tables = [far[k]] + [w[1, k] for w in w2[1:4]]
        for h in range(2):
            rows = slice(4 * h, 4 * h + 4)
            ends = [w[1, 2 * k + h] for w in (w2[0], w2[4])]
            part = merged(*[x[rows] for x in tables], *ends)
            total = part if total is None else total + part
    return jnp.sum(total, keepdims=True) * (1.0 / cells)


def up(m, flat, w2, s1, s0, u, mean, out, scratch):
    v1, t1, c1 = s1
    v0, t0, c0 = s0
    u2, t2, va, vb, c2, u3, t3, e3, f3, c3, rows, v1b, v1c, v0b, v0c = scratch
    n2, n3 = CHUNK, CHUNK // 2
    g2, g3 = ghosts_of(n2), ghosts_of(n3)
    par2, par3 = parity(W2, 4), parity(W2 // 2, 8)

    def load(a):
        for field, ref in ((0, t2),) + (() if flat else ((1, u2), (2, va))):
            row = 0
            for piece in w2:
                n = piece.shape[2]
                x = piece[field, a]
                ref[a + 1, row : row + n, :] = x - 16.0 * mean if flat else x
                row += n
        if flat:
            va[a + 1] = jnp.where(par2 == (a & 1), t2[a + 1] * (-1.0 / 6.0), 0.0)

    for a in range(n2):
        load(a)
    g2(va)
    if flat:
        c2 = c3 = None
    else:
        g2(u2)
        planes(1, n2 + 1, W2, lambda i: coef_of(c2, i, hessian(u2, i, 4), 0.0625)[1])
    half(vb, va, t2, c2, par2, 0, 4, 1, n2 + 1, g2)
    less0 = less1 = 0.0
    if flat:
        less0, less1 = mean, 4.0 * mean

    def first_sweep(par, scale, i):
        if not flat:
            return 0.0
        return jnp.where(par == (i & 1), (scale / 6.0) * mean, (scale / 3.0) * mean)

    def coarse(a):
        t = 0.5 * restrict(lambda k: t2[k] - jacobian(vb, k, 4, c2), 2 * a + 1, 4, rows, 2 * a, 0, 16)
        stores = [(t3, a + 1, t)]
        if not flat:
            x = 0.125 * restrict(lambda k: u2[k], 2 * a + 1, 4, rows, 2 * a + 1, 0, 16)
            stores.append((u3, a + 1, x))
        return stores

    planes(0, n3, 40, coarse)
    if not flat:
        g3(u3)

    def first(i):
        rho, stores = 1.0 / 6.0, []
        if not flat:
            rho, stores = coef_of(c3, i, hessian(u3, i, 8), 0.015625)
        return stores + [(e3, i, jnp.where(par3 == ((i + 1) & 1), -t3[i] * rho, 0.0))]

    planes(1, n3 + 1, W2 // 2, first)
    g3(e3)
    half(f3, e3, t3, c3, par3, 0, 8, 1, n3 + 1, g3)
    half(e3, f3, t3, c3, par3, 1, 8, 1, n3 + 1, g3)
    half(f3, e3, t3, c3, par3, 0, 8, 1, n3 + 1)

    for a in range(n3):
        double_rows(f3[a + 1], rows, a)
        e = rows[a, pl.ds(0, W2), :]
        va[2 * a + 1] = vb[2 * a + 1] + e
        va[2 * a + 2] = vb[2 * a + 2] + e
    g2(va)
    half(vb, va, t2, c2, par2, 1, 4, 1, n2 + 1, g2)
    half(va, vb, t2, c2, par2, 0, 4, 1, n2 + 1)

    par1 = parity(W1, 2)
    par0 = parity(BLOCK + 2 * m, 1)
    for x in range(W1 // 2):
        k = x + 10
        double_rows(spread(va[(k & 7) + 1], k >> 3), rows, x)
        e = rows[x, pl.ds(20, W1), :]
        v1b[2 * x] = v1[2 * x] + (e + first_sweep(par1, 4.0, 0))
        v1b[2 * x + 1] = v1[2 * x + 1] + (e + first_sweep(par1, 4.0, 1))
    r1 = m // 2
    half(v1c, v1b, t1, c1, par1, 0, 2, 8 - r1, 16 + r1, None, less1)
    half(v1b, v1c, t1, c1, par1, 1, 2, 9 - r1, 15 + r1, None, less1)

    w = BLOCK + 2 * m

    def raise0(a):
        double_rows(v1b[8 - m // 2 + a], rows, a)
        e = rows[a, pl.ds(16 - m, w), :]
        return [
            (v0b, 2 * a + k, v0[2 * a + k] + (e + first_sweep(par0, 1.0, k))) for k in range(2)
        ]

    planes(1, w // 2 - 1, w, raise0)
    half(v0c, v0b, t0, c0, par0, 0, 1, 3, w - 3, None, less0)
    inv = 1.0 / mean if flat else None

    def final(a):
        i = a + 4
        c = v0c[i]
        rho = 1.0 / 6.0 if flat else c0[6, i]
        new = c + (jacobian(v0c, i, 1, c0) - (t0[i] - less0)) * rho
        new = jnp.where(par0 == ((i + 1) & 1), new, c)
        new = new * inv if flat else new + u[i]
        return [(out, a, new[4 : w - 4])]

    planes(0, w - 8, w, final)


def turn_end(m, cells, turn, *refs):
    refs = list(refs)

    def take(n):
        got = refs[:n]
        del refs[:n]
        return got

    flat, ends = turn == 0, turn == len(MARGINS) - 1
    w2 = take(5)
    if flat:
        far, d, v1, t1, v0 = take(5)
        s1, s0, u = (v1, t1, None), (v0, d, None), None
    else:
        inv, d = (None, None) if ends else take(2)
        s1, s0, (u,) = take(3), take(3), take(1)
    (out,) = take(1)
    mean = None
    if flat:
        (inv,) = take(1)
        mean = mean_of(w2, far, cells)
        inv[...] = jnp.broadcast_to(1.0 / mean, inv.shape)
    msg, v, t, coef = (None,) * 4 if ends else take(4)
    up(m, flat, w2, s1, s0, u, mean, out, refs[:15])
    if not ends:
        down0(m - 4, inv, out, d, msg, v, t, coef, refs[15], refs[10])


def f32(*shape):
    return jax.ShapeDtypeStruct(shape, jnp.float32)


def scr(*shape):
    return pltpu.VMEM(shape, jnp.float32)


def call(body, name, outs, scratch, args):
    specs = [pl.BlockSpec(memory_space=VMEM)] * len(args)
    return pl.pallas_call(
        body,
        out_shape=outs,
        in_specs=specs,
        out_specs=[pl.BlockSpec(memory_space=VMEM)] * len(outs),
        scratch_shapes=scratch,
        interpret=INTERPRET,
        compiler_params=pltpu.CompilerParams(vmem_limit_bytes=16 << 20),
        name=name,
    )(*args)


def shift(x, axis, by):
    n = lax.axis_size(axis)
    return lax.ppermute(x, axis, [((i + by) % n, i) for i in range(n)])


def neighbours(x, axis, dim, width):
    n = x.shape[dim]
    before = shift(lax.slice_in_dim(x, n - width, n, axis=dim), axis, -1)
    after = shift(lax.slice_in_dim(x, 0, width, axis=dim), axis, 1)
    return before, x, after


def wide(x, lo, hi, axis):
    return shift(lo, axis, -3), shift(x, axis, -2), x, shift(x, axis, 2), shift(hi, axis, 3)


def per_device(density):
    cells = float(density.size * lax.axis_size("gx") * lax.axis_size("gy"))
    m = MARGINS[0]
    w = BLOCK + 2 * m
    n = BLOCK + 2
    own, lo, hi = call(
        pack_density, "pack", [f32(n, BLOCK, LANES), f32(n, m, LANES), f32(n, m, LANES)], [], [density]
    )
    d = jnp.concatenate([shift(hi, "gy", -1), own, shift(lo, "gy", 1)], 1)
    rows = scr(24, 64, LANES)
    msg, d, v0 = call(
        functools.partial(start, m),
        "start",
        [f32(10, 8, LANES)] + [f32(w, w, LANES)] * 2,
        [scr(w, w, LANES), rows],
        neighbours(d, "gx", 0, m + 2),
    )
    for turn, m in enumerate(MARGINS):
        flat, ends = turn == 0, turn == len(MARGINS) - 1
        w = BLOCK + 2 * m
        extra = 2 if flat else 0
        w1 = jnp.concatenate(neighbours(msg, "gy", 1, 8), 1)
        outs = [f32(8 + extra, 8, LANES)] + [f32(4 + extra, 8, LANES)] * 2
        outs += [f32(2, 8, LANES)] * (1 if flat else 0) + [f32(W1, W1, LANES)] * 2
        scratch = [scr(W1, W1, LANES)]
        if not flat:
            outs.append(f32(7, W1, W1, LANES))
            scratch += [scr(W1, W1, LANES), scr(12, 16, LANES)]
        got = call(
            functools.partial(down1, flat),
            f"down1_{turn}",
            outs,
            scratch + [rows],
            neighbours(w1, "gx", 0, w1.shape[0]),
        )
        fields = 2 if flat else 3
        outs = [f32(fields, 8, 8, LANES)] + [f32(fields, 8, 4, LANES)] * 2
        args = wide(*got[:3], "gx")
        if flat:
            args = (*args, shift(got[3], "gx", 8))
            outs.append(f32(2, 8, LANES))
            s1 = got[4:]
        else:
            s1 = got[3:]
        got = call(functools.partial(repack, flat), f"repack_{turn}", outs, [], args)
        args = list(wide(*got[:3], "gy"))
        if flat:
            args += [shift(got[3], "gy", 8), d, *s1, v0]
        else:
            args += ([] if ends else [inv, d]) + [*s1, *s0, u]
        a2 = scr(CHUNK + 2, W2, LANES)
        a3 = scr(CHUNK // 2 + 2, W2 // 2, LANES)
        scratch = [a2, a2, a2, a2, scr(7, CHUNK + 2, W2, LANES)]
        scratch += [a3, a3, a3, a3, scr(7, CHUNK // 2 + 2, W2 // 2, LANES)]
        scratch += [rows] + [scr(W1, W1, LANES)] * 2 + [scr(w, w, LANES)] * 2
        n = w - 8
        outs = [f32(n, n, LANES)] + ([f32(8, LANES)] if flat else [])
        if not ends:
            outs += [f32(8, 8, LANES), f32(n, n, LANES), f32(n, n, LANES), f32(7, n, n, LANES)]
            scratch += [scr(n, n, LANES)]
        u, *got = call(functools.partial(turn_end, m, cells, turn), f"up_{turn}", outs, scratch, args)
        if flat:
            inv, *got = got
        if not ends:
            msg, *s0 = got
    return u


def solution(mesh):
    spec = P("gx", "gy", None)
    return jax.shard_map(per_device, mesh=mesh, in_specs=(spec,), out_specs=spec, check_vma=False)
```

```python
import functools

import jax
import jax.numpy as jnp
from jax import lax
from jax.experimental import pallas as pl
from jax.experimental.pallas import tpu as pltpu
from jax.sharding import PartitionSpec as P


INTERPRET = False
LANES = 128
BLOCK = 16
MARGINS = (12, 8, 4)
FIELDS = (1, 3, 2)
W1 = 24
W2 = 32
CHUNK = 8
VMEM = pltpu.MemorySpace.VMEM
SMEM = pltpu.MemorySpace.SMEM
GROUP = 28


def roll(x, shift, axis):
    return pltpu.roll(x, shift % x.shape[axis], axis)


def iota(shape, axis):
    return lax.broadcasted_iota(jnp.int32, shape, axis)


def parity(rows, zs):
    shape = (rows, LANES)
    return (iota(shape, 0) + iota(shape, 1) // zs) & 1


def pures(v, i, zs):
    c, p, m = v[i], v[i + 1], v[i - 1]
    yp, ym = roll(c, -1, 0), roll(c, 1, 0)
    c2 = 2.0 * c
    xx = p + m - c2
    yy = yp + ym - c2
    zz = roll(c, -zs, 1) + roll(c, zs, 1) - c2
    return xx, yy, zz, p - m, yp - ym


def hessian(v, i, zs):
    xx, yy, zz, d, e = pures(v, i, zs)
    xy = roll(d, -1, 0) - roll(d, 1, 0)
    xz = roll(d, -zs, 1) - roll(d, zs, 1)
    yz = roll(e, -zs, 1) - roll(e, zs, 1)
    return xx, yy, zz, xy, xz, yz


def jacobian(v, i, zs, coef):
    if coef is None:
        xx, yy, zz, _, _ = pures(v, i, zs)
        return xx + yy + zz
    parts = hessian(v, i, zs)
    out = coef[0, i] * parts[0]
    for n in range(1, 6):
        out = out + coef[n, i] * parts[n]
    return out


def coef_of(coef, i, parts, s):
    xx, yy, zz, xy, xz, yz = parts
    g = 0.2 * s
    h = -0.025 * s
    rho = relax_of(xx, yy, zz, s)
    values = (1.0 + g * (yy + zz), 1.0 + g * (xx + zz), 1.0 + g * (xx + yy), h * xy, h * xz, h * yz, rho)
    return rho, [(coef, (n, i), value) for n, value in enumerate(values)]


def relax_of(xx, yy, zz, s):
    return 1.0 / jnp.maximum(6.0 + (0.8 * s) * (xx + yy + zz), 3.0)


def loop(lo, hi, f):
    def step(i, carry):
        f(i)
        return carry

    lax.fori_loop(lo, hi, step, 0)


def group_size(count, most):
    if count <= most:
        return count
    best = max(k for k in range(1, most + 1) if count % k == 0)
    return best if 2 * best > most else most


def planes(lo, hi, rows, f):
    many = group_size(hi - lo, GROUP // (rows // 8))

    def group(first, count):
        done = [f(first + k) for k in range(count)]
        for stores in done:
            for ref, i, value in stores:
                ref[i] = value

    def step(g, carry):
        group(lo + g * many, many)
        return carry

    whole = (hi - lo) // many
    lax.fori_loop(0, whole, step, 0)
    if (hi - lo) % many:
        group(lo + whole * many, (hi - lo) % many)


def half(dst, src, t, coef, par, color, zs, lo, hi, ghosts=None, less=0.0):
    def f(i):
        c = src[i]
        rho = 1.0 / 6.0 if coef is None else coef[6, i]
        new = c + (jacobian(src, i, zs, coef) - (t[i] - less)) * rho
        return [(dst, i, jnp.where(par == ((i + color) & 1), new, c))]

    planes(lo, hi, par.shape[0], f)
    if ghosts:
        ghosts(dst)


def pair_z(s, zs):
    even = (iota(s.shape, 1) // zs) & 1 == 0
    return s + jnp.where(even, roll(s, -zs, 1), roll(s, zs, 1))


def restrict(plane, i, zs, rows, slot, row0, n):
    s = pair_z(plane(i) + plane(i + 1), zs)
    slot = jnp.int32(slot)
    rows[slot, pl.ds(0, s.shape[0]), :] = s
    return rows[slot, pl.ds(row0, n, stride=2), :] + rows[slot, pl.ds(row0 + 1, n, stride=2), :]


def double_rows(x, rows, slot):
    n = x.shape[0]
    slot = jnp.int32(slot)
    rows[slot, pl.ds(0, n, stride=2), :] = x
    rows[slot, pl.ds(1, n, stride=2), :] = x


def down0(m, inv, u, d, msg, v, t, coef, va, rows):
    w = BLOCK + 2 * m
    cut = MARGINS[0] - m
    flat = coef is None
    par = parity(w, 1)

    def first(i):
        if flat:
            return [(va, i, jnp.where(par == (i & 1), d[i] * (-1.0 / 6.0), 0.0))]
        target = d[i + cut, cut : cut + w, :] * inv[0:1, :] - 1.0
        parts = hessian(u, i, 1)
        xx, yy, zz, xy, xz, yz = parts
        rho, stores = coef_of(coef, i, parts, 1.0)
        cubic = xx * yy + xx * zz + yy * zz - 0.0625 * (xy * xy + xz * xz + yz * yz)
        target = target - (xx + yy + zz) - 0.2 * cubic
        red = jnp.where(par == (i & 1), -target * rho, 0.0)
        return stores + [(t, i, target), (va, i, red)]

    edge = 0 if flat else 1
    planes(edge, w - edge, w, first)
    half(v, va, t, coef, par, 1, 1, edge + 1, w - edge - 1)
    lane_even = iota((8, LANES), 1) & 1 == 0

    def last(a):
        i = m + 2 * a
        t1 = 0.5 * restrict(lambda k: t[k] - jacobian(v, k, 1, coef), i, 1, rows, 2 * a, m, 8)
        if flat:
            u1 = jnp.zeros_like(t1)
        else:
            u1 = 0.125 * restrict(lambda k: u[k], i, 1, rows, 2 * a + 1, m, 8)
        return [(msg, a, jnp.where(lane_even, t1, u1))]

    planes(0, 8, 32, last)


def merged(*tables):
    out = tables[0]
    for x in tables[1:]:
        out = jnp.maximum(out, x)
    return out


def pack_density(density, own, lo, hi, known):
    m = MARGINS[0]
    half_block = BLOCK // 2
    total = jnp.sum(jnp.sum(density[...], axis=0), keepdims=True)
    for k in range(BLOCK):
        p = k if k < half_block else k + 2
        x = density[k]
        own[p] = x
        lo[p] = x[0:m]
        hi[p] = x[BLOCK - m : BLOCK]
    row = iota((BLOCK, LANES), 0)
    lane = iota((BLOCK, LANES), 1)
    for k in range(2):
        here = (row + 8 * k == lax.axis_index("gx")) & (lane == lax.axis_index("gy")) & (row < 8)
        table = jnp.where(here, total, 0.0)
        own[half_block + k] = table
        known[k] = table[0:8]
        lo[half_block + k] = table[0:m]
        hi[half_block + k] = table[0:m]


def join(before, own, after, far, out):
    m, half_block = MARGINS[0], BLOCK // 2
    for k in range(BLOCK + 2):
        out[k, 0:m, :] = before[k]
        out[k, m : m + BLOCK, :] = own[k]
        out[k, m + BLOCK :, :] = after[k]
    for k in range(2):
        out[half_block + k, m + 8 : m + 16, :] = far[k]


def start(m, db, do, da, far, msg, d, v, va, rows):
    half_block = BLOCK // 2
    for k in range(BLOCK):
        d[k + m] = do[k if k < half_block else k + 2]
    skip = BLOCK - m
    for k in range(m):
        d[k] = db[k if k + skip < half_block else k + 2]
        d[k + m + BLOCK] = da[k if k < half_block else k + 2]
    down0(m, None, None, d, msg, v, d, None, va, rows)
    for k in range(2):
        tables = []
        for ref, first in ((db, half_block - skip), (do, half_block), (da, half_block), (far, 0)):
            for row in (0, m, m + 8, m + BLOCK):
                tables.append(ref[first + k, row : row + 8, :])
        msg[8 + k] = merged(*tables)


def down1(turn, *refs):
    flat, lean = turn == 0, turn == len(MARGINS) - 1
    wb, wo, wa, msg, lo, hi, v, t = refs[:8]
    coef = u2 = None
    if flat:
        va, rows = refs[8:]
    elif lean:
        coef, va, u1, rows = refs[8:]
    else:
        coef, va, u1, u2, rows = refs[8:]
    par = parity(W1, 2)
    even = iota((W1, LANES), 1) & 1 == 0

    def unpack(a):
        stores = []
        for k, w in enumerate((wb, wo, wa)):
            i = a + 8 * k
            p = w[a]
            target = jnp.where(even, p, roll(p, 1, 1))
            stores.append((t, i, target))
            if flat:
                stores.append((va, i, jnp.where(par == (i & 1), target * (-1.0 / 6.0), 0.0)))
            else:
                stores.append((u1, i, jnp.where(even, roll(p, -1, 1), p)))
        return stores

    planes(0, 8, 40, unpack)
    if not flat:

        def first(i):
            rho, stores = coef_of(coef, i, hessian(u1, i, 2), 0.25)
            return stores + [(va, i, jnp.where(par == (i & 1), -t[i] * rho, 0.0))]

        planes(1, W1 - 1, W1, first)

    if u2 is not None:

        def coarse(a):
            u = 0.125 * restrict(lambda k: u1[k], 2 * a, 2, rows, a, 0, 12)
            return [(u2, (a, slice(0, 12)), u)]

        planes(0, 12, W1, coarse)
    half(v, va, t, coef, par, 1, 2, 1 if flat else 3, W1 - (1 if flat else 3))
    phase = iota((8, LANES), 1) & 3
    par2 = parity(8, 4)

    def last(a):
        t2 = 0.5 * restrict(lambda k: t[k] - jacobian(v, k, 2, coef), 4 + 2 * a, 2, rows, 2 * a, 4, 8)
        if flat:
            return [(msg, a, t2)]
        if lean:
            u = 0.125 * restrict(lambda k: u1[k], 4 + 2 * a, 2, rows, 2 * a + 1, 4, 8)
            return [(msg, a, jnp.where(phase == 1, u, t2))]
        xx, yy, zz, _, _ = pures(u2, a + 2, 4)
        rho = relax_of(xx, yy, zz, 0.0625)
        rows[2 * a + 1, pl.ds(0, 16), :] = rho
        red = jnp.where(par2 == (a & 1), -t2 * rows[2 * a + 1, pl.ds(2, 8), :], 0.0)
        uc = u2[a + 2, 2:10, :]
        return [(msg, a, jnp.where(phase == 1, uc, jnp.where(phase == 2, red, t2)))]

    planes(0, 8, 32, last)
    lo[0:4] = msg[0:4]
    hi[0:4] = msg[4:8]
    if flat:
        for k in range(2):
            table = merged(*[w[8 + k, 8 * j : 8 * j + 8, :] for w in (wb, wo, wa) for j in range(3)])
            msg[8 + k] = table
            lo[4 + k] = table
            hi[4 + k] = table


def repack(turn, w0, w1, w2, w3, w4, out, lo, hi):
    if turn == 0:
        for k in range(2):
            table = merged(*[w[w.shape[0] - 2 + k] for w in (w0, w1, w2, w3, w4)])
            out[8 + k] = table
            for ref in (lo, hi):
                ref[8 + 2 * k] = table[0:4]
                ref[9 + 2 * k] = table[4:8]
    phase = iota((8, LANES), 1) & 3
    where_from = [(w0, k) for k in range(4)]
    for w in (w1, w2, w3):
        where_from += [(w, k) for k in range(8)]
    where_from += [(w4, k) for k in range(4)]
    for a in range(CHUNK):
        for field in range(FIELDS[turn]):
            got = None
            for c in range(4):
                ref, k = where_from[a + CHUNK * c]
                part = ref[k]
                part = roll(part, c - field, 1) if c != field else part
                got = part if got is None else jnp.where(phase == c, part, got)
            out[CHUNK * field + a] = got
            lo[CHUNK * field + a] = got[0:4]
            hi[CHUNK * field + a] = got[4:8]


def ghosts_of(n):
    def fill(v):
        v[0] = roll(v[n], 1, 1)
        v[n + 1] = roll(v[1], -1, 1)

    return fill


def spread(x, c):
    phase = iota(x.shape, 1) & 3
    x = jnp.where(phase == c, x, 0.0)
    x = x + roll(x, -1 if c & 1 else 1, 1)
    return x + roll(x, -2 if c & 2 else 2, 1)


def mean_of(w2, cells):
    total = None
    for k in range(2):
        for h in range(2):
            tables = [w[8 + k, 4 * h : 4 * h + 4, :] for w in w2[1:4]]
            part = merged(*tables, w2[0][8 + 2 * k + h], w2[4][8 + 2 * k + h])
            total = part if total is None else total + part
    return jnp.sum(total, keepdims=True) * (1.0 / cells)


def up(m, turn, w2, s1, s0, u, mean, out, scratch):
    flat = turn == 0
    v1, t1, c1 = s1
    v0, t0, c0 = s0
    u2, t2, va, vb, c2, u3, t3, e3, f3, c3, rows, v1b, v1c, v0b, v0c = scratch
    n2, n3 = CHUNK, CHUNK // 2
    g2, g3 = ghosts_of(n2), ghosts_of(n3)
    par2, par3 = parity(W2, 4), parity(W2 // 2, 8)

    def load(a):
        for field, ref in enumerate((t2, u2, va)[: FIELDS[turn]]):
            row = 0
            for piece in w2:
                n = piece.shape[1]
                x = piece[CHUNK * field + a]
                ref[a + 1, row : row + n, :] = x - 16.0 * mean if flat else x
                row += n
        if flat:
            va[a + 1] = jnp.where(par2 == (a & 1), t2[a + 1] * (-1.0 / 6.0), 0.0)

    for a in range(n2):
        load(a)
    if flat:
        c2 = c3 = None
    else:
        g2(u2)

        def first2(i):
            rho, stores = coef_of(c2, i, hessian(u2, i, 4), 0.0625)
            if FIELDS[turn] == 2:
                stores.append((va, i, jnp.where(par2 == ((i + 1) & 1), -t2[i] * rho, 0.0)))
            return stores

        planes(1, n2 + 1, W2, first2)
    g2(va)
    half(vb, va, t2, c2, par2, 0, 4, 1, n2 + 1, g2)
    less0 = less1 = 0.0
    if flat:
        less0, less1 = mean, 4.0 * mean

    def first_sweep(par, scale, i):
        if not flat:
            return 0.0
        return jnp.where(par == (i & 1), (scale / 6.0) * mean, (scale / 3.0) * mean)

    def coarse(a):
        t = 0.5 * restrict(lambda k: t2[k] - jacobian(vb, k, 4, c2), 2 * a + 1, 4, rows, 2 * a, 0, 16)
        stores = [(t3, a + 1, t)]
        if not flat:
            x = 0.125 * restrict(lambda k: u2[k], 2 * a + 1, 4, rows, 2 * a + 1, 0, 16)
            stores.append((u3, a + 1, x))
        return stores

    planes(0, n3, 40, coarse)
    if not flat:
        g3(u3)

    def first(i):
        rho, stores = 1.0 / 6.0, []
        if not flat:
            rho, stores = coef_of(c3, i, hessian(u3, i, 8), 0.015625)
        return stores + [(e3, i, jnp.where(par3 == ((i + 1) & 1), -t3[i] * rho, 0.0))]

    planes(1, n3 + 1, W2 // 2, first)
    g3(e3)
    half(f3, e3, t3, c3, par3, 0, 8, 1, n3 + 1, g3)
    half(e3, f3, t3, c3, par3, 1, 8, 1, n3 + 1, g3)
    half(f3, e3, t3, c3, par3, 0, 8, 1, n3 + 1)

    for a in range(n3):
        double_rows(f3[a + 1], rows, a)
        e = rows[a, pl.ds(0, W2), :]
        va[2 * a + 1] = vb[2 * a + 1] + e
        va[2 * a + 2] = vb[2 * a + 2] + e
    g2(va)
    half(vb, va, t2, c2, par2, 1, 4, 1, n2 + 1, g2)
    half(va, vb, t2, c2, par2, 0, 4, 1, n2 + 1)

    par1 = parity(W1, 2)
    par0 = parity(BLOCK + 2 * m, 1)
    for x in range(W1 // 2):
        k = x + 10
        double_rows(spread(va[(k & 7) + 1], k >> 3), rows, x)
        e = rows[x, pl.ds(20, W1), :]
        v1b[2 * x] = v1[2 * x] + (e + first_sweep(par1, 4.0, 0))
        v1b[2 * x + 1] = v1[2 * x + 1] + (e + first_sweep(par1, 4.0, 1))
    r1 = m // 2
    half(v1c, v1b, t1, c1, par1, 0, 2, 8 - r1, 16 + r1, None, less1)
    half(v1b, v1c, t1, c1, par1, 1, 2, 9 - r1, 15 + r1, None, less1)

    w = BLOCK + 2 * m

    def raise0(a):
        double_rows(v1b[8 - m // 2 + a], rows, a)
        e = rows[a, pl.ds(16 - m, w), :]
        return [
            (v0b, 2 * a + k, v0[2 * a + k] + (e + first_sweep(par0, 1.0, k))) for k in range(2)
        ]

    planes(1, w // 2 - 1, w, raise0)
    half(v0c, v0b, t0, c0, par0, 0, 1, 3, w - 3, None, less0)
    inv = 1.0 / mean if flat else None

    def final(a):
        i = a + 4
        c = v0c[i]
        rho = 1.0 / 6.0 if flat else c0[6, i]
        new = c + (jacobian(v0c, i, 1, c0) - (t0[i] - less0)) * rho
        new = jnp.where(par0 == ((i + 1) & 1), new, c)
        new = new * inv if flat else new + u[i]
        return [(out, a, new[4 : w - 4])]

    planes(0, w - 8, w, final)


def turn_end(m, cells, turn, *refs):
    refs = list(refs)

    def take(n):
        got = refs[:n]
        del refs[:n]
        return got

    flat, ends = turn == 0, turn == len(MARGINS) - 1
    w2 = take(5)
    if flat:
        d, v1, t1, v0 = take(4)
        s1, s0, u = (v1, t1, None), (v0, d, None), None
    else:
        inv, d = (None, None) if ends else take(2)
        s1, s0, (u,) = take(3), take(3), take(1)
    (out,) = take(1)
    mean = None
    if flat:
        (inv,) = take(1)
        mean = mean_of(w2, cells)
        inv[...] = jnp.broadcast_to(1.0 / mean, inv.shape)
    msg, v, t, coef = (None,) * 4 if ends else take(4)
    up(m, turn, w2, s1, s0, u, mean, out, refs[:15])
    if not ends:
        down0(m - 4, inv, out, d, msg, v, t, coef, refs[15], refs[10])


def f32(*shape):
    return jax.ShapeDtypeStruct(shape, jnp.float32)


def scr(*shape):
    return pltpu.VMEM(shape, jnp.float32)


def call(body, name, outs, scratch, args):
    specs = [pl.BlockSpec(memory_space=VMEM)] * len(args)
    return pl.pallas_call(
        body,
        out_shape=outs,
        in_specs=specs,
        out_specs=[pl.BlockSpec(memory_space=VMEM)] * len(outs),
        scratch_shapes=scratch,
        interpret=INTERPRET,
        compiler_params=pltpu.CompilerParams(vmem_limit_bytes=16 << 20),
        name=name,
    )(*args)


def shift(x, axis, by):
    n = lax.axis_size(axis)
    return lax.ppermute(x, axis, [((i + by) % n, i) for i in range(n)])


def neighbours(x, axis, dim, width):
    n = x.shape[dim]
    before = shift(lax.slice_in_dim(x, n - width, n, axis=dim), axis, -1)
    after = shift(lax.slice_in_dim(x, 0, width, axis=dim), axis, 1)
    return before, x, after


def wide(x, lo, hi, axis):
    if axis == "gx":
        ends = shift(lo, axis, -3), shift(hi, axis, 3)
    else:
        ends = shift(hi, axis, -4), shift(lo, axis, 4)
    return ends[0], shift(x, axis, -2), x, shift(x, axis, 2), ends[1]


def per_device(density):
    cells = float(density.size * lax.axis_size("gx") * lax.axis_size("gy"))
    m = MARGINS[0]
    w = BLOCK + 2 * m
    n = BLOCK + 2
    outs = [f32(n, BLOCK, LANES), f32(n, m, LANES), f32(n, m, LANES), f32(2, 8, LANES)]
    own, lo, hi, known = call(pack_density, "pack", outs, [], [density])
    args = [shift(hi, "gy", -1), own, shift(lo, "gy", 1), shift(known, "gy", 8)]
    (d,) = call(join, "join", [f32(n, w, LANES)], [], args)
    far = shift(d[BLOCK // 2 : BLOCK // 2 + 2], "gx", 8)
    rows = scr(24, 64, LANES)
    msg, d, v0 = call(
        functools.partial(start, m),
        "start",
        [f32(10, 8, LANES)] + [f32(w, w, LANES)] * 2,
        [scr(w, w, LANES), rows],
        [*neighbours(d, "gx", 0, m + 2), far],
    )
    for turn, m in enumerate(MARGINS):
        flat, ends = turn == 0, turn == len(MARGINS) - 1
        w = BLOCK + 2 * m
        extra = 2 if flat else 0
        w1 = jnp.concatenate(neighbours(msg, "gy", 1, 8), 1)
        outs = [f32(8 + extra, 8, LANES)] + [f32(4 + extra, 8, LANES)] * 2
        outs += [f32(W1, W1, LANES)] * 2
        scratch = [scr(W1, W1, LANES)]
        if not flat:
            outs.append(f32(7, W1, W1, LANES))
            scratch += [scr(W1, W1, LANES)] + ([] if ends else [scr(12, 16, LANES)])
        msg, lo, hi, *s1 = call(
            functools.partial(down1, turn),
            f"down1_{turn}",
            outs,
            scratch + [rows],
            neighbours(w1, "gx", 0, w1.shape[0]),
        )
        size = CHUNK * FIELDS[turn]
        outs = [f32(size + extra, 8, LANES)] + [f32(size + 2 * extra, 4, LANES)] * 2
        got = call(functools.partial(repack, turn), f"repack_{turn}", outs, [], wide(msg, lo, hi, "gx"))
        args = list(wide(*got, "gy"))
        if flat:
            args += [d, *s1, v0]
        else:
            args += ([] if ends else [inv, d]) + [*s1, *s0, u]
        a2 = scr(CHUNK + 2, W2, LANES)
        a3 = scr(CHUNK // 2 + 2, W2 // 2, LANES)
        scratch = [a2, a2, a2, a2, scr(7, CHUNK + 2, W2, LANES)]
        scratch += [a3, a3, a3, a3, scr(7, CHUNK // 2 + 2, W2 // 2, LANES)]
        scratch += [rows] + [scr(W1, W1, LANES)] * 2 + [scr(w, w, LANES)] * 2
        n = w - 8
        outs = [f32(n, n, LANES)] + ([f32(8, LANES)] if flat else [])
        if not ends:
            outs += [f32(8, 8, LANES), f32(n, n, LANES), f32(n, n, LANES), f32(7, n, n, LANES)]
            scratch += [scr(n, n, LANES)]
        u, *got = call(functools.partial(turn_end, m, cells, turn), f"up_{turn}", outs, scratch, args)
        if flat:
            inv, *got = got
        if not ends:
            msg, *s0 = got
    return u


def solution(mesh):
    spec = P("gx", "gy", None)
    return jax.shard_map(per_device, mesh=mesh, in_specs=(spec,), out_specs=spec, check_vma=False)
```

```python
import functools

import jax
import jax.numpy as jnp
from jax import lax
from jax.experimental import pallas as pl
from jax.experimental.pallas import tpu as pltpu
from jax.sharding import PartitionSpec as P


INTERPRET = False
LANES = 128
BLOCK = 16
MARGINS = (12, 8, 4)
FIELDS = (1, 3, 2)
W1 = 24
W2 = 32
CHUNK = 8
VMEM = pltpu.MemorySpace.VMEM
SMEM = pltpu.MemorySpace.SMEM
GROUP = 32


def roll(x, shift, axis):
    return pltpu.roll(x, shift % x.shape[axis], axis)


def iota(shape, axis):
    return lax.broadcasted_iota(jnp.int32, shape, axis)


def parity(rows, zs):
    shape = (rows, LANES)
    return (iota(shape, 0) + iota(shape, 1) // zs) & 1


class Place:
    def __init__(self, base, scale=1, offset=0):
        self.base, self.scale, self.offset = base, scale, offset

    def __add__(self, n):
        return Place(self.base, self.scale, self.offset + n)

    __radd__ = __add__

    def __sub__(self, n):
        return self + (-n)

    def __mul__(self, n):
        return Place(self.base, self.scale * n, self.offset * n)

    __rmul__ = __mul__

    def __and__(self, n):
        return self.value() & n

    def value(self):
        return self.base * self.scale + self.offset


SHARED = {}


def number(i):
    return i.value() if isinstance(i, Place) else i


def shared(kind, v, i, make):
    if not isinstance(i, Place):
        return make()
    key = (kind, id(v), i.scale, i.offset)
    if key not in SHARED:
        SHARED[key] = make()
    return SHARED[key]


def at(v, i):
    return shared("plane", v, i, lambda: v[number(i)])


def across(v, i, step, axis):
    def make():
        c = at(v, i)
        after, before = roll(c, -step, axis), roll(c, step, axis)
        return after + before, after - before

    return shared(axis, v, i, make)


def pures(v, i, zs):
    c2 = 2.0 * at(v, i)
    xx = at(v, i + 1) + at(v, i - 1) - c2
    return xx, across(v, i, 1, 0)[0] - c2, across(v, i, zs, 1)[0] - c2


def hessian(v, i, zs):
    xx, yy, zz = pures(v, i, zs)
    xy = across(v, i + 1, 1, 0)[1] - across(v, i - 1, 1, 0)[1]
    xz = across(v, i + 1, zs, 1)[1] - across(v, i - 1, zs, 1)[1]
    dz = across(v, i, zs, 1)[1]
    yz = roll(dz, -1, 0) - roll(dz, 1, 0)
    return xx, yy, zz, xy, xz, yz


def jacobian(v, i, zs, coef):
    if coef is None:
        around = across(v, i, 1, 0)[0] + across(v, i, zs, 1)[0]
        return at(v, i + 1) + at(v, i - 1) + around - 6.0 * at(v, i)
    parts = hessian(v, i, zs)
    k = number(i)
    out = coef[0, k] * parts[0]
    for n in range(1, 6):
        out = out + coef[n, k] * parts[n]
    return out


def coef_of(coef, i, parts, s):
    xx, yy, zz, xy, xz, yz = parts
    g = 0.2 * s
    h = -0.025 * s
    rho = relax_of(xx, yy, zz, s)
    values = (1.0 + g * (yy + zz), 1.0 + g * (xx + zz), 1.0 + g * (xx + yy), h * xy, h * xz, h * yz, rho)
    return rho, [(coef, (n, i), value) for n, value in enumerate(values)]


def relax_of(xx, yy, zz, s):
    return 1.0 / jnp.maximum(6.0 + (0.8 * s) * (xx + yy + zz), 3.0)


def loop(lo, hi, f):
    def step(i, carry):
        f(i)
        return carry

    lax.fori_loop(lo, hi, step, 0)


def group_size(count, most):
    if count <= most:
        return count
    best = max(k for k in range(1, most + 1) if count % k == 0)
    return best if 2 * best > most else most


def planes(lo, hi, rows, f):
    many = group_size(hi - lo, GROUP // (rows // 8))

    def group(first, count):
        SHARED.clear()
        done = [f(Place(first) + k) for k in range(count)]
        SHARED.clear()
        for stores in done:
            for ref, i, value in stores:
                ref[tuple(map(number, i)) if isinstance(i, tuple) else number(i)] = value

    def step(g, carry):
        group(lo + g * many, many)
        return carry

    whole = (hi - lo) // many
    lax.fori_loop(0, whole, step, 0)
    if (hi - lo) % many:
        group(lo + whole * many, (hi - lo) % many)


def half(dst, src, t, coef, par, color, zs, lo, hi, ghosts=None, less=0.0):
    def f(i):
        c = at(src, i)
        rho = 1.0 / 6.0 if coef is None else coef[6, number(i)]
        new = c + (jacobian(src, i, zs, coef) - (at(t, i) - less)) * rho
        return [(dst, i, jnp.where(par == ((i + color) & 1), new, c))]

    planes(lo, hi, par.shape[0], f)
    if ghosts:
        ghosts(dst)


def pair_z(s, zs):
    even = (iota(s.shape, 1) // zs) & 1 == 0
    return s + jnp.where(even, roll(s, -zs, 1), roll(s, zs, 1))


def restrict(plane, i, zs, rows, slot, row0, n):
    s = pair_z(plane(i) + plane(i + 1), zs)
    slot = jnp.int32(number(slot))
    rows[slot, pl.ds(0, s.shape[0]), :] = s
    return rows[slot, pl.ds(row0, n, stride=2), :] + rows[slot, pl.ds(row0 + 1, n, stride=2), :]


def double_rows(x, rows, slot):
    n = x.shape[0]
    slot = jnp.int32(number(slot))
    rows[slot, pl.ds(0, n, stride=2), :] = x
    rows[slot, pl.ds(1, n, stride=2), :] = x


def down0(m, inv, u, d, msg, v, t, coef, va, rows):
    w = BLOCK + 2 * m
    cut = MARGINS[0] - m
    flat = coef is None
    par = parity(w, 1)

    def first(i):
        if flat:
            return [(va, i, jnp.where(par == (i & 1), at(d, i) * (-1.0 / 6.0), 0.0))]
        target = d[number(i + cut), cut : cut + w, :] * inv[0:1, :] - 1.0
        parts = hessian(u, i, 1)
        xx, yy, zz, xy, xz, yz = parts
        rho, stores = coef_of(coef, i, parts, 1.0)
        cubic = xx * yy + xx * zz + yy * zz - 0.0625 * (xy * xy + xz * xz + yz * yz)
        target = target - (xx + yy + zz) - 0.2 * cubic
        red = jnp.where(par == (i & 1), -target * rho, 0.0)
        return stores + [(t, i, target), (va, i, red)]

    edge = 0 if flat else 1
    planes(edge, w - edge, w, first)
    half(v, va, t, coef, par, 1, 1, edge + 1, w - edge - 1)
    lane_even = iota((8, LANES), 1) & 1 == 0

    def last(a):
        i = m + 2 * a
        t1 = 0.5 * restrict(lambda k: at(t, k) - jacobian(v, k, 1, coef), i, 1, rows, 2 * a, m, 8)
        if flat:
            u1 = jnp.zeros_like(t1)
        else:
            u1 = 0.125 * restrict(lambda k: at(u, k), i, 1, rows, 2 * a + 1, m, 8)
        return [(msg, a, jnp.where(lane_even, t1, u1))]

    planes(0, 8, 32, last)


def merged(*tables):
    out = tables[0]
    for x in tables[1:]:
        out = jnp.maximum(out, x)
    return out


def pack_density(density, own, lo, hi, known):
    m = MARGINS[0]
    half_block = BLOCK // 2
    total = jnp.sum(jnp.sum(density[...], axis=0), keepdims=True)
    for k in range(BLOCK):
        p = k if k < half_block else k + 2
        x = density[k]
        own[p] = x
        lo[p] = x[0:m]
        hi[p] = x[BLOCK - m : BLOCK]
    row = iota((BLOCK, LANES), 0)
    lane = iota((BLOCK, LANES), 1)
    for k in range(2):
        here = (row + 8 * k == lax.axis_index("gx")) & (lane == lax.axis_index("gy")) & (row < 8)
        table = jnp.where(here, total, 0.0)
        own[half_block + k] = table
        known[k] = table[0:8]
        lo[half_block + k] = table[0:m]
        hi[half_block + k] = table[0:m]


def join(before, own, after, far, out):
    m, half_block = MARGINS[0], BLOCK // 2
    for k in range(BLOCK + 2):
        out[k, 0:m, :] = before[k]
        out[k, m : m + BLOCK, :] = own[k]
        out[k, m + BLOCK :, :] = after[k]
    for k in range(2):
        out[half_block + k, m + 8 : m + 16, :] = far[k]


def start(m, db, do, da, far, msg, d, v, va, rows):
    half_block = BLOCK // 2
    for k in range(BLOCK):
        d[k + m] = do[k if k < half_block else k + 2]
    skip = BLOCK - m
    for k in range(m):
        d[k] = db[k if k + skip < half_block else k + 2]
        d[k + m + BLOCK] = da[k if k < half_block else k + 2]
    down0(m, None, None, d, msg, v, d, None, va, rows)
    for k in range(2):
        tables = []
        for ref, first in ((db, half_block - skip), (do, half_block), (da, half_block), (far, 0)):
            for row in (0, m, m + 8, m + BLOCK):
                tables.append(ref[first + k, row : row + 8, :])
        msg[8 + k] = merged(*tables)


def down1(turn, *refs):
    flat, lean = turn == 0, turn == len(MARGINS) - 1
    wb, wo, wa, msg, lo, hi, v, t = refs[:8]
    coef = u2 = None
    if flat:
        va, rows = refs[8:]
    elif lean:
        coef, va, u1, rows = refs[8:]
    else:
        coef, va, u1, u2, rows = refs[8:]
    par = parity(W1, 2)
    even = iota((W1, LANES), 1) & 1 == 0

    def unpack(a):
        stores = []
        for k, w in enumerate((wb, wo, wa)):
            i = a + 8 * k
            p = at(w, a)
            target = jnp.where(even, p, roll(p, 1, 1))
            stores.append((t, i, target))
            if flat:
                stores.append((va, i, jnp.where(par == (i & 1), target * (-1.0 / 6.0), 0.0)))
            else:
                stores.append((u1, i, jnp.where(even, roll(p, -1, 1), p)))
        return stores

    planes(0, 8, 40, unpack)
    if not flat:

        def first(i):
            rho, stores = coef_of(coef, i, hessian(u1, i, 2), 0.25)
            return stores + [(va, i, jnp.where(par == (i & 1), -at(t, i) * rho, 0.0))]

        planes(1, W1 - 1, W1, first)

    if u2 is not None:

        def coarse(a):
            u = 0.125 * restrict(lambda k: at(u1, k), 2 * a, 2, rows, a, 0, 12)
            return [(u2, (a, slice(0, 12)), u)]

        planes(0, 12, W1, coarse)
    half(v, va, t, coef, par, 1, 2, 1 if flat else 3, W1 - (1 if flat else 3))
    phase = iota((8, LANES), 1) & 3
    par2 = parity(8, 4)

    def last(a):
        t2 = 0.5 * restrict(lambda k: at(t, k) - jacobian(v, k, 2, coef), 4 + 2 * a, 2, rows, 2 * a, 4, 8)
        if flat:
            return [(msg, a, t2)]
        if lean:
            u = 0.125 * restrict(lambda k: at(u1, k), 4 + 2 * a, 2, rows, 2 * a + 1, 4, 8)
            return [(msg, a, jnp.where(phase == 1, u, t2))]
        xx, yy, zz = pures(u2, a + 2, 4)
        rho = relax_of(xx, yy, zz, 0.0625)
        slot = number(2 * a + 1)
        rows[slot, pl.ds(0, 16), :] = rho
        red = jnp.where(par2 == (a & 1), -t2 * rows[slot, pl.ds(2, 8), :], 0.0)
        uc = u2[number(a + 2), 2:10, :]
        return [(msg, a, jnp.where(phase == 1, uc, jnp.where(phase == 2, red, t2)))]

    planes(0, 8, 32, last)
    lo[0:4] = msg[0:4]
    hi[0:4] = msg[4:8]
    if flat:
        for k in range(2):
            table = merged(*[w[8 + k, 8 * j : 8 * j + 8, :] for w in (wb, wo, wa) for j in range(3)])
            msg[8 + k] = table
            lo[4 + k] = table
            hi[4 + k] = table


def repack(turn, w0, w1, w2, w3, w4, out, lo, hi):
    if turn == 0:
        for k in range(2):
            table = merged(*[w[w.shape[0] - 2 + k] for w in (w0, w1, w2, w3, w4)])
            out[8 + k] = table
            for ref in (lo, hi):
                ref[8 + 2 * k] = table[0:4]
                ref[9 + 2 * k] = table[4:8]
    phase = iota((8, LANES), 1) & 3
    where_from = [(w0, k) for k in range(4)]
    for w in (w1, w2, w3):
        where_from += [(w, k) for k in range(8)]
    where_from += [(w4, k) for k in range(4)]
    for a in range(CHUNK):
        for field in range(FIELDS[turn]):
            got = None
            for c in range(4):
                ref, k = where_from[a + CHUNK * c]
                part = ref[k]
                part = roll(part, c - field, 1) if c != field else part
                got = part if got is None else jnp.where(phase == c, part, got)
            out[CHUNK * field + a] = got
            lo[CHUNK * field + a] = got[0:4]
            hi[CHUNK * field + a] = got[4:8]


def ghosts_of(n):
    def fill(v):
        v[0] = roll(v[n], 1, 1)
        v[n + 1] = roll(v[1], -1, 1)

    return fill


def spread(x, c):
    phase = iota(x.shape, 1) & 3
    x = jnp.where(phase == c, x, 0.0)
    x = x + roll(x, -1 if c & 1 else 1, 1)
    return x + roll(x, -2 if c & 2 else 2, 1)


def mean_of(w2, cells):
    total = None
    for k in range(2):
        for h in range(2):
            tables = [w[8 + k, 4 * h : 4 * h + 4, :] for w in w2[1:4]]
            part = merged(*tables, w2[0][8 + 2 * k + h], w2[4][8 + 2 * k + h])
            total = part if total is None else total + part
    return jnp.sum(total, keepdims=True) * (1.0 / cells)


def up(m, turn, w2, s1, s0, u, mean, out, scratch):
    flat = turn == 0
    v1, t1, c1 = s1
    v0, t0, c0 = s0
    u2, t2, va, vb, c2, u3, t3, e3, f3, c3, rows, v1b, v1c, v0b, v0c = scratch
    n2, n3 = CHUNK, CHUNK // 2
    g2, g3 = ghosts_of(n2), ghosts_of(n3)
    par2, par3 = parity(W2, 4), parity(W2 // 2, 8)

    def load(a):
        for field, ref in enumerate((t2, u2, va)[: FIELDS[turn]]):
            row = 0
            for piece in w2:
                n = piece.shape[1]
                x = piece[CHUNK * field + a]
                ref[a + 1, row : row + n, :] = x - 16.0 * mean if flat else x
                row += n
        if flat:
            va[a + 1] = jnp.where(par2 == (a & 1), t2[a + 1] * (-1.0 / 6.0), 0.0)

    for a in range(n2):
        load(a)
    if flat:
        c2 = c3 = None
    else:
        g2(u2)

        def first2(i):
            rho, stores = coef_of(c2, i, hessian(u2, i, 4), 0.0625)
            if FIELDS[turn] == 2:
                stores.append((va, i, jnp.where(par2 == ((i + 1) & 1), -at(t2, i) * rho, 0.0)))
            return stores

        planes(1, n2 + 1, W2, first2)
    g2(va)
    half(vb, va, t2, c2, par2, 0, 4, 1, n2 + 1, g2)
    less0 = less1 = 0.0
    if flat:
        less0, less1 = mean, 4.0 * mean

    def first_sweep(par, scale, i):
        if not flat:
            return 0.0
        return jnp.where(par == (i & 1), (scale / 6.0) * mean, (scale / 3.0) * mean)

    def coarse(a):
        t = 0.5 * restrict(lambda k: at(t2, k) - jacobian(vb, k, 4, c2), 2 * a + 1, 4, rows, 2 * a, 0, 16)
        stores = [(t3, a + 1, t)]
        if not flat:
            x = 0.125 * restrict(lambda k: at(u2, k), 2 * a + 1, 4, rows, 2 * a + 1, 0, 16)
            stores.append((u3, a + 1, x))
        return stores

    planes(0, n3, 40, coarse)
    if not flat:
        g3(u3)

    def first(i):
        rho, stores = 1.0 / 6.0, []
        if not flat:
            rho, stores = coef_of(c3, i, hessian(u3, i, 8), 0.015625)
        return stores + [(e3, i, jnp.where(par3 == ((i + 1) & 1), -at(t3, i) * rho, 0.0))]

    planes(1, n3 + 1, W2 // 2, first)
    g3(e3)
    half(f3, e3, t3, c3, par3, 0, 8, 1, n3 + 1, g3)
    half(e3, f3, t3, c3, par3, 1, 8, 1, n3 + 1, g3)
    half(f3, e3, t3, c3, par3, 0, 8, 1, n3 + 1)

    for a in range(n3):
        double_rows(f3[a + 1], rows, a)
        e = rows[a, pl.ds(0, W2), :]
        va[2 * a + 1] = vb[2 * a + 1] + e
        va[2 * a + 2] = vb[2 * a + 2] + e
    g2(va)
    half(vb, va, t2, c2, par2, 1, 4, 1, n2 + 1, g2)
    half(va, vb, t2, c2, par2, 0, 4, 1, n2 + 1)

    par1 = parity(W1, 2)
    par0 = parity(BLOCK + 2 * m, 1)
    for x in range(W1 // 2):
        k = x + 10
        double_rows(spread(va[(k & 7) + 1], k >> 3), rows, x)
        e = rows[x, pl.ds(20, W1), :]
        v1b[2 * x] = v1[2 * x] + (e + first_sweep(par1, 4.0, 0))
        v1b[2 * x + 1] = v1[2 * x + 1] + (e + first_sweep(par1, 4.0, 1))
    r1 = m // 2
    half(v1c, v1b, t1, c1, par1, 0, 2, 8 - r1, 16 + r1, None, less1)
    half(v1b, v1c, t1, c1, par1, 1, 2, 9 - r1, 15 + r1, None, less1)

    w = BLOCK + 2 * m

    def raise0(a):
        double_rows(at(v1b, 8 - m // 2 + a), rows, a)
        e = rows[number(a), pl.ds(16 - m, w), :]
        return [
            (v0b, 2 * a + k, at(v0, 2 * a + k) + (e + first_sweep(par0, 1.0, k))) for k in range(2)
        ]

    planes(1, w // 2 - 1, w, raise0)
    half(v0c, v0b, t0, c0, par0, 0, 1, 3, w - 3, None, less0)
    inv = 1.0 / mean if flat else None

    def final(a):
        i = a + 4
        c = at(v0c, i)
        rho = 1.0 / 6.0 if flat else c0[6, number(i)]
        new = c + (jacobian(v0c, i, 1, c0) - (at(t0, i) - less0)) * rho
        new = jnp.where(par0 == ((i + 1) & 1), new, c)
        new = new * inv if flat else new + at(u, i)
        return [(out, a, new[4 : w - 4])]

    planes(0, w - 8, w, final)


def turn_end(m, cells, turn, *refs):
    refs = list(refs)

    def take(n):
        got = refs[:n]
        del refs[:n]
        return got

    flat, ends = turn == 0, turn == len(MARGINS) - 1
    w2 = take(5)
    if flat:
        d, v1, t1, v0 = take(4)
        s1, s0, u = (v1, t1, None), (v0, d, None), None
    else:
        inv, d = (None, None) if ends else take(2)
        s1, s0, (u,) = take(3), take(3), take(1)
    (out,) = take(1)
    mean = None
    if flat:
        (inv,) = take(1)
        mean = mean_of(w2, cells)
        inv[...] = jnp.broadcast_to(1.0 / mean, inv.shape)
    msg, v, t, coef = (None,) * 4 if ends else take(4)
    up(m, turn, w2, s1, s0, u, mean, out, refs[:15])
    if not ends:
        down0(m - 4, inv, out, d, msg, v, t, coef, refs[15], refs[10])


def f32(*shape):
    return jax.ShapeDtypeStruct(shape, jnp.float32)


def scr(*shape):
    return pltpu.VMEM(shape, jnp.float32)


def call(body, name, outs, scratch, args):
    specs = [pl.BlockSpec(memory_space=VMEM)] * len(args)
    return pl.pallas_call(
        body,
        out_shape=outs,
        in_specs=specs,
        out_specs=[pl.BlockSpec(memory_space=VMEM)] * len(outs),
        scratch_shapes=scratch,
        interpret=INTERPRET,
        compiler_params=pltpu.CompilerParams(vmem_limit_bytes=16 << 20),
        name=name,
    )(*args)


def shift(x, axis, by):
    n = lax.axis_size(axis)
    return lax.ppermute(x, axis, [((i + by) % n, i) for i in range(n)])


def neighbours(x, axis, dim, width):
    n = x.shape[dim]
    before = shift(lax.slice_in_dim(x, n - width, n, axis=dim), axis, -1)
    after = shift(lax.slice_in_dim(x, 0, width, axis=dim), axis, 1)
    return before, x, after


def wide(x, lo, hi, axis):
    if axis == "gx":
        ends = shift(lo, axis, -3), shift(hi, axis, 3)
    else:
        ends = shift(hi, axis, -4), shift(lo, axis, 4)
    return ends[0], shift(x, axis, -2), x, shift(x, axis, 2), ends[1]


def per_device(density):
    cells = float(density.size * lax.axis_size("gx") * lax.axis_size("gy"))
    m = MARGINS[0]
    w = BLOCK + 2 * m
    n = BLOCK + 2
    outs = [f32(n, BLOCK, LANES), f32(n, m, LANES), f32(n, m, LANES), f32(2, 8, LANES)]
    own, lo, hi, known = call(pack_density, "pack", outs, [], [density])
    args = [shift(hi, "gy", -1), own, shift(lo, "gy", 1), shift(known, "gy", 8)]
    (d,) = call(join, "join", [f32(n, w, LANES)], [], args)
    far = shift(d[BLOCK // 2 : BLOCK // 2 + 2], "gx", 8)
    rows = scr(24, 64, LANES)
    msg, d, v0 = call(
        functools.partial(start, m),
        "start",
        [f32(10, 8, LANES)] + [f32(w, w, LANES)] * 2,
        [scr(w, w, LANES), rows],
        [*neighbours(d, "gx", 0, m + 2), far],
    )
    for turn, m in enumerate(MARGINS):
        flat, ends = turn == 0, turn == len(MARGINS) - 1
        w = BLOCK + 2 * m
        extra = 2 if flat else 0
        w1 = jnp.concatenate(neighbours(msg, "gy", 1, 8), 1)
        outs = [f32(8 + extra, 8, LANES)] + [f32(4 + extra, 8, LANES)] * 2
        outs += [f32(W1, W1, LANES)] * 2
        scratch = [scr(W1, W1, LANES)]
        if not flat:
            outs.append(f32(7, W1, W1, LANES))
            scratch += [scr(W1, W1, LANES)] + ([] if ends else [scr(12, 16, LANES)])
        msg, lo, hi, *s1 = call(
            functools.partial(down1, turn),
            f"down1_{turn}",
            outs,
            scratch + [rows],
            neighbours(w1, "gx", 0, w1.shape[0]),
        )
        size = CHUNK * FIELDS[turn]
        outs = [f32(size + extra, 8, LANES)] + [f32(size + 2 * extra, 4, LANES)] * 2
        got = call(functools.partial(repack, turn), f"repack_{turn}", outs, [], wide(msg, lo, hi, "gx"))
        args = list(wide(*got, "gy"))
        if flat:
            args += [d, *s1, v0]
        else:
            args += ([] if ends else [inv, d]) + [*s1, *s0, u]
        a2 = scr(CHUNK + 2, W2, LANES)
        a3 = scr(CHUNK // 2 + 2, W2 // 2, LANES)
        scratch = [a2, a2, a2, a2, scr(7, CHUNK + 2, W2, LANES)]
        scratch += [a3, a3, a3, a3, scr(7, CHUNK // 2 + 2, W2 // 2, LANES)]
        scratch += [rows] + [scr(W1, W1, LANES)] * 2 + [scr(w, w, LANES)] * 2
        n = w - 8
        outs = [f32(n, n, LANES)] + ([f32(8, LANES)] if flat else [])
        if not ends:
            outs += [f32(8, 8, LANES), f32(n, n, LANES), f32(n, n, LANES), f32(7, n, n, LANES)]
            scratch += [scr(n, n, LANES)]
        u, *got = call(functools.partial(turn_end, m, cells, turn), f"up_{turn}", outs, scratch, args)
        if flat:
            inv, *got = got
        if not ends:
            msg, *s0 = got
    return u


def solution(mesh):
    spec = P("gx", "gy", None)
    return jax.shard_map(per_device, mesh=mesh, in_specs=(spec,), out_specs=spec, check_vma=False)
```

```python
import functools

import jax
import jax.numpy as jnp
from jax import lax
from jax.experimental import pallas as pl
from jax.experimental.pallas import tpu as pltpu
from jax.sharding import PartitionSpec as P


INTERPRET = False
LANES = 128
BLOCK = 16
MARGINS = (12, 8, 4)
FIELDS = (1, 3, 2)
W1 = 24
W2 = 32
CHUNK = 8
VMEM = pltpu.MemorySpace.VMEM
SMEM = pltpu.MemorySpace.SMEM
GROUP = 32


def roll(x, shift, axis):
    return pltpu.roll(x, shift % x.shape[axis], axis)


def iota(shape, axis):
    return lax.broadcasted_iota(jnp.int32, shape, axis)


def parity(rows, zs):
    shape = (rows, LANES)
    return (iota(shape, 0) + iota(shape, 1) // zs) & 1


class Place:
    def __init__(self, base, scale=1, offset=0):
        self.base, self.scale, self.offset = base, scale, offset

    def __add__(self, n):
        return Place(self.base, self.scale, self.offset + n)

    __radd__ = __add__

    def __sub__(self, n):
        return self + (-n)

    def __mul__(self, n):
        return Place(self.base, self.scale * n, self.offset * n)

    __rmul__ = __mul__

    def __and__(self, n):
        return self.value() & n

    def value(self):
        return self.base * self.scale + self.offset


SHARED = {}


def number(i):
    return i.value() if isinstance(i, Place) else i


def shared(kind, v, i, make):
    if not isinstance(i, Place):
        return make()
    key = (kind, id(v), i.scale, i.offset)
    if key not in SHARED:
        SHARED[key] = make()
    return SHARED[key]


def at(v, i):
    return shared("plane", v, i, lambda: v[number(i)])


def across(v, i, step, axis):
    def make():
        c = at(v, i)
        after, before = roll(c, -step, axis), roll(c, step, axis)
        return after + before, after - before

    return shared(axis, v, i, make)


def pures(v, i, zs):
    c2 = 2.0 * at(v, i)
    xx = at(v, i + 1) + at(v, i - 1) - c2
    return xx, across(v, i, 1, 0)[0] - c2, across(v, i, zs, 1)[0] - c2


def hessian(v, i, zs):
    xx, yy, zz = pures(v, i, zs)
    xy = across(v, i + 1, 1, 0)[1] - across(v, i - 1, 1, 0)[1]
    xz = across(v, i + 1, zs, 1)[1] - across(v, i - 1, zs, 1)[1]
    dz = across(v, i, zs, 1)[1]
    yz = roll(dz, -1, 0) - roll(dz, 1, 0)
    return xx, yy, zz, xy, xz, yz


def jacobian(v, i, zs, coef):
    if coef is None:
        around = across(v, i, 1, 0)[0] + across(v, i, zs, 1)[0]
        return at(v, i + 1) + at(v, i - 1) + around - 6.0 * at(v, i)
    parts = hessian(v, i, zs)
    k = number(i)
    out = coef[0, k] * parts[0]
    for n in range(1, 6):
        out = out + coef[n, k] * parts[n]
    return out


def coef_of(coef, i, parts, s):
    xx, yy, zz, xy, xz, yz = parts
    g = 0.2 * s
    h = -0.025 * s
    rho = relax_of(xx, yy, zz, s)
    values = (1.0 + g * (yy + zz), 1.0 + g * (xx + zz), 1.0 + g * (xx + yy), h * xy, h * xz, h * yz, rho)
    return rho, [(coef, (n, i), value) for n, value in enumerate(values)]


def relax_of(xx, yy, zz, s):
    return 1.0 / jnp.maximum(6.0 + (0.8 * s) * (xx + yy + zz), 3.0)


def loop(lo, hi, f):
    def step(i, carry):
        f(i)
        return carry

    lax.fori_loop(lo, hi, step, 0)


def group_size(count, most):
    if count <= most:
        return count
    best = max(k for k in range(1, most + 1) if count % k == 0)
    return best if 2 * best > most else most


def planes(lo, hi, rows, f):
    many = group_size(hi - lo, GROUP // (rows // 8))

    def group(first, count):
        SHARED.clear()
        done = [f(Place(first) + k) for k in range(count)]
        SHARED.clear()
        for stores in done:
            for ref, i, value in stores:
                ref[tuple(map(number, i)) if isinstance(i, tuple) else number(i)] = value

    def step(g, carry):
        group(lo + g * many, many)
        return carry

    whole = (hi - lo) // many
    lax.fori_loop(0, whole, step, 0)
    if (hi - lo) % many:
        group(lo + whole * many, (hi - lo) % many)


def half(dst, src, t, coef, par, color, zs, lo, hi, ghosts=None, less=0.0):
    def f(i):
        c = at(src, i)
        rho = 1.0 / 6.0 if coef is None else coef[6, number(i)]
        new = c + (jacobian(src, i, zs, coef) - (at(t, i) - less)) * rho
        return [(dst, i, jnp.where(par == ((i + color) & 1), new, c))]

    planes(lo, hi, par.shape[0], f)
    if ghosts:
        ghosts(dst)


def pair_z(s, zs):
    even = (iota(s.shape, 1) // zs) & 1 == 0
    return s + jnp.where(even, roll(s, -zs, 1), roll(s, zs, 1))


def restrict(plane, i, zs, rows, slot, row0, n):
    s = pair_z(plane(i) + plane(i + 1), zs)
    slot = jnp.int32(number(slot))
    rows[slot, pl.ds(0, s.shape[0]), :] = s
    return rows[slot, pl.ds(row0, n, stride=2), :] + rows[slot, pl.ds(row0 + 1, n, stride=2), :]


def double_rows(x, rows, slot):
    n = x.shape[0]
    slot = jnp.int32(number(slot))
    rows[slot, pl.ds(0, n, stride=2), :] = x
    rows[slot, pl.ds(1, n, stride=2), :] = x


def down0(m, inv, u, d, msg, v, t, coef, va, rows):
    w = BLOCK + 2 * m
    cut = MARGINS[0] - m
    flat = coef is None
    par = parity(w, 1)

    def first(i):
        if flat:
            return [(va, i, jnp.where(par == (i & 1), at(d, i) * (-1.0 / 6.0), 0.0))]
        target = d[number(i + cut), cut : cut + w, :] * inv[0:1, :] - 1.0
        parts = hessian(u, i, 1)
        xx, yy, zz, xy, xz, yz = parts
        rho, stores = coef_of(coef, i, parts, 1.0)
        cubic = xx * yy + xx * zz + yy * zz - 0.0625 * (xy * xy + xz * xz + yz * yz)
        target = target - (xx + yy + zz) - 0.2 * cubic
        red = jnp.where(par == (i & 1), -target * rho, 0.0)
        return stores + [(t, i, target), (va, i, red)]

    edge = 0 if flat else 1
    planes(edge, w - edge, w, first)
    half(v, va, t, coef, par, 1, 1, edge + 1, w - edge - 1)
    lane_even = iota((8, LANES), 1) & 1 == 0

    def last(a):
        i = m + 2 * a
        t1 = 0.5 * restrict(lambda k: at(t, k) - jacobian(v, k, 1, coef), i, 1, rows, 2 * a, m, 8)
        if flat:
            u1 = jnp.zeros_like(t1)
        else:
            u1 = 0.125 * restrict(lambda k: at(u, k), i, 1, rows, 2 * a + 1, m, 8)
        return [(msg, a, jnp.where(lane_even, t1, u1))]

    planes(0, 8, 32, last)


def merged(*tables):
    out = tables[0]
    for x in tables[1:]:
        out = jnp.maximum(out, x)
    return out


def pack_density(density, own, lo, hi, known):
    m = MARGINS[0]
    half_block = BLOCK // 2
    total = jnp.sum(jnp.sum(density[...], axis=0), keepdims=True)
    for k in range(BLOCK):
        p = k if k < half_block else k + 2
        x = density[k]
        own[p] = x
        lo[p] = x[0:m]
        hi[p] = x[BLOCK - m : BLOCK]
    row = iota((BLOCK, LANES), 0)
    lane = iota((BLOCK, LANES), 1)
    for k in range(2):
        here = (row + 8 * k == lax.axis_index("gx")) & (lane == lax.axis_index("gy")) & (row < 8)
        table = jnp.where(here, total, 0.0)
        own[half_block + k] = table
        known[k] = table[0:8]
        lo[half_block + k] = table[0:m]
        hi[half_block + k] = table[0:m]


def join(before, own, after, far, out):
    m, half_block = MARGINS[0], BLOCK // 2
    for k in range(BLOCK + 2):
        out[k, 0:m, :] = before[k]
        out[k, m : m + BLOCK, :] = own[k]
        out[k, m + BLOCK :, :] = after[k]
    for k in range(2):
        out[half_block + k, m + 8 : m + 16, :] = far[k]


def start(m, db, do, da, far, msg, d, v, va, rows):
    half_block = BLOCK // 2
    for k in range(BLOCK):
        d[k + m] = do[k if k < half_block else k + 2]
    skip = BLOCK - m
    for k in range(m):
        d[k] = db[k if k + skip < half_block else k + 2]
        d[k + m + BLOCK] = da[k if k < half_block else k + 2]
    down0(m, None, None, d, msg, v, d, None, va, rows)
    for k in range(2):
        tables = []
        for ref, first in ((db, half_block - skip), (do, half_block), (da, half_block), (far, 0)):
            for row in (0, m, m + 8, m + BLOCK):
                tables.append(ref[first + k, row : row + 8, :])
        msg[8 + k] = merged(*tables)


def down1(turn, *refs):
    flat, lean = turn == 0, turn == len(MARGINS) - 1
    wb, wo, wa, msg, lo, hi, v, t = refs[:8]
    coef = u2 = None
    if flat:
        va, rows = refs[8:]
    elif lean:
        coef, va, u1, rows = refs[8:]
    else:
        coef, va, u1, u2, rows = refs[8:]
    par = parity(W1, 2)
    even = iota((W1, LANES), 1) & 1 == 0

    def unpack(a):
        stores = []
        for k, w in enumerate((wb, wo, wa)):
            i = a + 8 * k
            p = at(w, a)
            target = jnp.where(even, p, roll(p, 1, 1))
            stores.append((t, i, target))
            if flat:
                stores.append((va, i, jnp.where(par == (i & 1), target * (-1.0 / 6.0), 0.0)))
            else:
                stores.append((u1, i, jnp.where(even, roll(p, -1, 1), p)))
        return stores

    planes(0, 8, 40, unpack)
    if not flat:

        def first(i):
            rho, stores = coef_of(coef, i, hessian(u1, i, 2), 0.25)
            return stores + [(va, i, jnp.where(par == (i & 1), -at(t, i) * rho, 0.0))]

        planes(1, W1 - 1, W1, first)

    if u2 is not None:

        def coarse(a):
            u = 0.125 * restrict(lambda k: at(u1, k), 2 * a, 2, rows, a, 0, 12)
            return [(u2, (a, slice(0, 12)), u)]

        planes(0, 12, W1, coarse)
    half(v, va, t, coef, par, 1, 2, 1 if flat else 3, W1 - (1 if flat else 3))
    phase = iota((8, LANES), 1) & 3
    par2 = parity(8, 4)

    def last(a):
        t2 = 0.5 * restrict(lambda k: at(t, k) - jacobian(v, k, 2, coef), 4 + 2 * a, 2, rows, 2 * a, 4, 8)
        if flat:
            return [(msg, a, t2)]
        if lean:
            u = 0.125 * restrict(lambda k: at(u1, k), 4 + 2 * a, 2, rows, 2 * a + 1, 4, 8)
            return [(msg, a, jnp.where(phase == 1, u, t2))]
        xx, yy, zz = pures(u2, a + 2, 4)
        rho = relax_of(xx, yy, zz, 0.0625)
        slot = number(2 * a + 1)
        rows[slot, pl.ds(0, 16), :] = rho
        red = jnp.where(par2 == (a & 1), -t2 * rows[slot, pl.ds(2, 8), :], 0.0)
        uc = u2[number(a + 2), 2:10, :]
        return [(msg, a, jnp.where(phase == 1, uc, jnp.where(phase == 2, red, t2)))]

    planes(0, 8, 32, last)
    lo[0:4] = msg[0:4]
    hi[0:4] = msg[4:8]
    if flat:
        for k in range(2):
            table = merged(*[w[8 + k, 8 * j : 8 * j + 8, :] for w in (wb, wo, wa) for j in range(3)])
            msg[8 + k] = table
            lo[4 + k] = table
            hi[4 + k] = table


def repack(turn, w0, w1, w2, w3, w4, out, lo, hi):
    if turn == 0:
        for k in range(2):
            table = merged(*[w[w.shape[0] - 2 + k] for w in (w0, w1, w2, w3, w4)])
            out[8 + k] = table
            for ref in (lo, hi):
                ref[8 + 2 * k] = table[0:4]
                ref[9 + 2 * k] = table[4:8]
    phase = iota((8, LANES), 1) & 3
    where_from = [(w0, k) for k in range(4)]
    for w in (w1, w2, w3):
        where_from += [(w, k) for k in range(8)]
    where_from += [(w4, k) for k in range(4)]
    for a in range(CHUNK):
        for field in range(FIELDS[turn]):
            got = None
            for c in range(4):
                ref, k = where_from[a + CHUNK * c]
                part = ref[k]
                part = roll(part, c - field, 1) if c != field else part
                got = part if got is None else jnp.where(phase == c, part, got)
            out[CHUNK * field + a] = got
            lo[CHUNK * field + a] = got[0:4]
            hi[CHUNK * field + a] = got[4:8]


def ghosts_of(n):
    def fill(v):
        v[0] = roll(v[n], 1, 1)
        v[n + 1] = roll(v[1], -1, 1)

    return fill


def spread(x, c):
    phase = iota(x.shape, 1) & 3
    x = jnp.where(phase == c, x, 0.0)
    x = x + roll(x, -1 if c & 1 else 1, 1)
    return x + roll(x, -2 if c & 2 else 2, 1)


def mean_of(w2, cells):
    total = None
    for k in range(2):
        for h in range(2):
            tables = [w[8 + k, 4 * h : 4 * h + 4, :] for w in w2[1:4]]
            part = merged(*tables, w2[0][8 + 2 * k + h], w2[4][8 + 2 * k + h])
            total = part if total is None else total + part
    return jnp.sum(total, keepdims=True) * (1.0 / cells)


def up(m, turn, w2, s1, s0, u, mean, out, scratch):
    flat = turn == 0
    v1, t1, c1 = s1
    v0, t0, c0 = s0
    u2, t2, va, vb, c2, u3, t3, e3, f3, c3, rows, v1b, v1c, v0b, v0c = scratch
    n2, n3 = CHUNK, CHUNK // 2
    g2, g3 = ghosts_of(n2), ghosts_of(n3)
    par2, par3 = parity(W2, 4), parity(W2 // 2, 8)

    def load(a):
        for field, ref in enumerate((t2, u2, va)[: FIELDS[turn]]):
            row = 0
            for piece in w2:
                n = piece.shape[1]
                x = piece[CHUNK * field + a]
                ref[a + 1, row : row + n, :] = x - 16.0 * mean if flat else x
                row += n
        if flat:
            va[a + 1] = jnp.where(par2 == (a & 1), t2[a + 1] * (-1.0 / 6.0), 0.0)

    for a in range(n2):
        load(a)
    if flat:
        c2 = c3 = None
    else:
        g2(u2)

        def first2(i):
            rho, stores = coef_of(c2, i, hessian(u2, i, 4), 0.0625)
            if FIELDS[turn] == 2:
                stores.append((va, i, jnp.where(par2 == ((i + 1) & 1), -at(t2, i) * rho, 0.0)))
            return stores

        planes(1, n2 + 1, W2, first2)
    g2(va)
    half(vb, va, t2, c2, par2, 0, 4, 1, n2 + 1, g2)
    less0 = less1 = 0.0
    if flat:
        less0, less1 = mean, 4.0 * mean

    def first_sweep(par, scale, i):
        if not flat:
            return 0.0
        return jnp.where(par == (i & 1), (scale / 6.0) * mean, (scale / 3.0) * mean)

    def coarse(a):
        t = 0.5 * restrict(lambda k: at(t2, k) - jacobian(vb, k, 4, c2), 2 * a + 1, 4, rows, 2 * a, 0, 16)
        stores = [(t3, a + 1, t)]
        if not flat:
            x = 0.125 * restrict(lambda k: at(u2, k), 2 * a + 1, 4, rows, 2 * a + 1, 0, 16)
            stores.append((u3, a + 1, x))
        return stores

    planes(0, n3, 40, coarse)
    if not flat:
        g3(u3)

    def first(i):
        rho, stores = 1.0 / 6.0, []
        if not flat:
            rho, stores = coef_of(c3, i, hessian(u3, i, 8), 0.015625)
        return stores + [(e3, i, jnp.where(par3 == ((i + 1) & 1), -at(t3, i) * rho, 0.0))]

    planes(1, n3 + 1, W2 // 2, first)
    g3(e3)
    half(f3, e3, t3, c3, par3, 0, 8, 1, n3 + 1, g3)
    half(e3, f3, t3, c3, par3, 1, 8, 1, n3 + 1, g3)
    half(f3, e3, t3, c3, par3, 0, 8, 1, n3 + 1)

    for a in range(n3):
        double_rows(f3[a + 1], rows, a)
        e = rows[a, pl.ds(0, W2), :]
        va[2 * a + 1] = vb[2 * a + 1] + e
        va[2 * a + 2] = vb[2 * a + 2] + e
    g2(va)
    half(vb, va, t2, c2, par2, 1, 4, 1, n2 + 1, g2)
    half(va, vb, t2, c2, par2, 0, 4, 1, n2 + 1)

    par1 = parity(W1, 2)
    par0 = parity(BLOCK + 2 * m, 1)
    for x in range(W1 // 2):
        k = x + 10
        double_rows(spread(va[(k & 7) + 1], k >> 3), rows, x)
        e = rows[x, pl.ds(20, W1), :]
        v1b[2 * x] = v1[2 * x] + (e + first_sweep(par1, 4.0, 0))
        v1b[2 * x + 1] = v1[2 * x + 1] + (e + first_sweep(par1, 4.0, 1))
    r1 = m // 2
    half(v1c, v1b, t1, c1, par1, 0, 2, 8 - r1, 16 + r1, None, less1)
    half(v1b, v1c, t1, c1, par1, 1, 2, 9 - r1, 15 + r1, None, less1)

    w = BLOCK + 2 * m

    def raise0(a):
        double_rows(at(v1b, 8 - m // 2 + a), rows, a)
        e = rows[number(a), pl.ds(16 - m, w), :]
        return [
            (v0b, 2 * a + k, at(v0, 2 * a + k) + (e + first_sweep(par0, 1.0, k))) for k in range(2)
        ]

    planes(1, w // 2 - 1, w, raise0)
    half(v0c, v0b, t0, c0, par0, 0, 1, 3, w - 3, None, less0)
    inv = 1.0 / mean if flat else None

    def final(a):
        i = a + 4
        c = at(v0c, i)
        rho = 1.0 / 6.0 if flat else c0[6, number(i)]
        new = c + (jacobian(v0c, i, 1, c0) - (at(t0, i) - less0)) * rho
        new = jnp.where(par0 == ((i + 1) & 1), new, c)
        new = new * inv if flat else new + at(u, i)
        return [(out, a, new[4 : w - 4])]

    planes(0, w - 8, w, final)


def turn_end(m, cells, turn, *refs):
    refs = list(refs)

    def take(n):
        got = refs[:n]
        del refs[:n]
        return got

    flat, ends = turn == 0, turn == len(MARGINS) - 1
    w2 = take(5)
    if flat:
        d, v1, t1, v0 = take(4)
        s1, s0, u = (v1, t1, None), (v0, d, None), None
    else:
        inv, d = (None, None) if ends else take(2)
        s1, s0, (u,) = take(3), take(3), take(1)
    (out,) = take(1)
    mean = None
    if flat:
        (inv,) = take(1)
        mean = mean_of(w2, cells)
        inv[...] = jnp.broadcast_to(1.0 / mean, inv.shape)
    msg, v, t, coef = (None,) * 4 if ends else take(4)
    up(m, turn, w2, s1, s0, u, mean, out, refs[:15])
    if not ends:
        down0(m - 4, inv, out, d, msg, v, t, coef, refs[15], refs[10])


def f32(*shape):
    return jax.ShapeDtypeStruct(shape, jnp.float32)


def scr(*shape):
    return pltpu.VMEM(shape, jnp.float32)


def call(body, name, outs, scratch, args):
    specs = [pl.BlockSpec(memory_space=VMEM)] * len(args)
    return pl.pallas_call(
        body,
        out_shape=outs,
        in_specs=specs,
        out_specs=[pl.BlockSpec(memory_space=VMEM)] * len(outs),
        scratch_shapes=scratch,
        interpret=INTERPRET,
        compiler_params=pltpu.CompilerParams(vmem_limit_bytes=16 << 20),
        name=name,
    )(*args)


def shift(x, axis, by):
    n = lax.axis_size(axis)
    return lax.ppermute(x, axis, [((i + by) % n, i) for i in range(n)])


def neighbours(x, axis, dim, width):
    n = x.shape[dim]
    before = shift(lax.slice_in_dim(x, n - width, n, axis=dim), axis, -1)
    after = shift(lax.slice_in_dim(x, 0, width, axis=dim), axis, 1)
    return before, x, after


def wide(x, lo, hi, axis):
    return shift(hi, axis, -4), shift(x, axis, -2), x, shift(x, axis, 2), shift(lo, axis, 4)


def per_device(density):
    cells = float(density.size * lax.axis_size("gx") * lax.axis_size("gy"))
    m = MARGINS[0]
    w = BLOCK + 2 * m
    n = BLOCK + 2
    outs = [f32(n, BLOCK, LANES), f32(n, m, LANES), f32(n, m, LANES), f32(2, 8, LANES)]
    own, lo, hi, known = call(pack_density, "pack", outs, [], [density])
    args = [shift(hi, "gy", -1), own, shift(lo, "gy", 1), shift(known, "gy", 4)]
    (d,) = call(join, "join", [f32(n, w, LANES)], [], args)
    far = shift(d[BLOCK // 2 : BLOCK // 2 + 2], "gx", 4)
    rows = scr(24, 64, LANES)
    msg, d, v0 = call(
        functools.partial(start, m),
        "start",
        [f32(10, 8, LANES)] + [f32(w, w, LANES)] * 2,
        [scr(w, w, LANES), rows],
        [*neighbours(d, "gx", 0, m + 2), far],
    )
    for turn, m in enumerate(MARGINS):
        flat, ends = turn == 0, turn == len(MARGINS) - 1
        w = BLOCK + 2 * m
        extra = 2 if flat else 0
        w1 = jnp.concatenate(neighbours(msg, "gy", 1, 8), 1)
        outs = [f32(8 + extra, 8, LANES)] + [f32(4 + extra, 8, LANES)] * 2
        outs += [f32(W1, W1, LANES)] * 2
        scratch = [scr(W1, W1, LANES)]
        if not flat:
            outs.append(f32(7, W1, W1, LANES))
            scratch += [scr(W1, W1, LANES)] + ([] if ends else [scr(12, 16, LANES)])
        msg, lo, hi, *s1 = call(
            functools.partial(down1, turn),
            f"down1_{turn}",
            outs,
            scratch + [rows],
            neighbours(w1, "gx", 0, w1.shape[0]),
        )
        size = CHUNK * FIELDS[turn]
        outs = [f32(size + extra, 8, LANES)] + [f32(size + 2 * extra, 4, LANES)] * 2
        got = call(functools.partial(repack, turn), f"repack_{turn}", outs, [], wide(msg, lo, hi, "gx"))
        args = list(wide(*got, "gy"))
        if flat:
            args += [d, *s1, v0]
        else:
            args += ([] if ends else [inv, d]) + [*s1, *s0, u]
        a2 = scr(CHUNK + 2, W2, LANES)
        a3 = scr(CHUNK // 2 + 2, W2 // 2, LANES)
        scratch = [a2, a2, a2, a2, scr(7, CHUNK + 2, W2, LANES)]
        scratch += [a3, a3, a3, a3, scr(7, CHUNK // 2 + 2, W2 // 2, LANES)]
        scratch += [rows] + [scr(W1, W1, LANES)] * 2 + [scr(w, w, LANES)] * 2
        n = w - 8
        outs = [f32(n, n, LANES)] + ([f32(8, LANES)] if flat else [])
        if not ends:
            outs += [f32(8, 8, LANES), f32(n, n, LANES), f32(n, n, LANES), f32(7, n, n, LANES)]
            scratch += [scr(n, n, LANES)]
        u, *got = call(functools.partial(turn_end, m, cells, turn), f"up_{turn}", outs, scratch, args)
        if flat:
            inv, *got = got
        if not ends:
            msg, *s0 = got
    return u


def solution(mesh):
    spec = P("gx", "gy", None)
    return jax.shard_map(per_device, mesh=mesh, in_specs=(spec,), out_specs=spec, check_vma=False)
```

```python
import functools

import jax
import jax.numpy as jnp
from jax import lax
from jax.experimental import pallas as pl
from jax.experimental.pallas import tpu as pltpu
from jax.sharding import PartitionSpec as P


INTERPRET = False
LANES = 128
BLOCK = 16
MARGINS = (12, 8, 4)
FIELDS = (1, 3, 2)
W1 = 24
W2 = 32
CHUNK = 8
VMEM = pltpu.MemorySpace.VMEM
SMEM = pltpu.MemorySpace.SMEM
GROUP = 32


def roll(x, shift, axis):
    return pltpu.roll(x, shift % x.shape[axis], axis)


def iota(shape, axis):
    return lax.broadcasted_iota(jnp.int32, shape, axis)


def parity(rows, zs):
    shape = (rows, LANES)
    return (iota(shape, 0) + iota(shape, 1) // zs) & 1


class Place:
    def __init__(self, base, scale=1, offset=0):
        self.base, self.scale, self.offset = base, scale, offset

    def __add__(self, n):
        return Place(self.base, self.scale, self.offset + n)

    __radd__ = __add__

    def __sub__(self, n):
        return self + (-n)

    def __mul__(self, n):
        return Place(self.base, self.scale * n, self.offset * n)

    __rmul__ = __mul__

    def __and__(self, n):
        return self.value() & n

    def value(self):
        return self.base * self.scale + self.offset


SHARED = {}


def number(i):
    return i.value() if isinstance(i, Place) else i


def shared(kind, v, i, make):
    if not isinstance(i, Place):
        return make()
    key = (kind, id(v), i.scale, i.offset)
    if key not in SHARED:
        SHARED[key] = make()
    return SHARED[key]


def at(v, i):
    return shared("plane", v, i, lambda: v[number(i)])


def across(v, i, step, axis):
    def make():
        c = at(v, i)
        after, before = roll(c, -step, axis), roll(c, step, axis)
        return after + before, after - before

    return shared(axis, v, i, make)


def pures(v, i, zs):
    c2 = 2.0 * at(v, i)
    xx = at(v, i + 1) + at(v, i - 1) - c2
    return xx, across(v, i, 1, 0)[0] - c2, across(v, i, zs, 1)[0] - c2


def hessian(v, i, zs):
    xx, yy, zz = pures(v, i, zs)
    xy = across(v, i + 1, 1, 0)[1] - across(v, i - 1, 1, 0)[1]
    xz = across(v, i + 1, zs, 1)[1] - across(v, i - 1, zs, 1)[1]
    dz = across(v, i, zs, 1)[1]
    yz = roll(dz, -1, 0) - roll(dz, 1, 0)
    return xx, yy, zz, xy, xz, yz


def jacobian(v, i, zs, coef):
    if coef is None:
        around = across(v, i, 1, 0)[0] + across(v, i, zs, 1)[0]
        return at(v, i + 1) + at(v, i - 1) + around - 6.0 * at(v, i)
    parts = hessian(v, i, zs)
    k = number(i)
    out = coef[0, k] * parts[0]
    for n in range(1, 6):
        out = out + coef[n, k] * parts[n]
    return out


def coef_of(coef, i, parts, s):
    xx, yy, zz, xy, xz, yz = parts
    g = 0.2 * s
    h = -0.025 * s
    rho = relax_of(xx, yy, zz, s)
    values = (1.0 + g * (yy + zz), 1.0 + g * (xx + zz), 1.0 + g * (xx + yy), h * xy, h * xz, h * yz, rho)
    return rho, [(coef, (n, i), value) for n, value in enumerate(values)]


def relax_of(xx, yy, zz, s):
    return 1.0 / jnp.maximum(6.0 + (0.8 * s) * (xx + yy + zz), 3.0)


def loop(lo, hi, f):
    def step(i, carry):
        f(i)
        return carry

    lax.fori_loop(lo, hi, step, 0)


def group_size(count, most):
    if count <= most:
        return count
    best = max(k for k in range(1, most + 1) if count % k == 0)
    return best if 2 * best > most else most


def planes(lo, hi, rows, f):
    many = group_size(hi - lo, GROUP // (rows // 8))

    def group(first, count):
        SHARED.clear()
        done = [f(Place(first) + k) for k in range(count)]
        SHARED.clear()
        for stores in done:
            for ref, i, value in stores:
                ref[tuple(map(number, i)) if isinstance(i, tuple) else number(i)] = value

    def step(g, carry):
        group(lo + g * many, many)
        return carry

    whole = (hi - lo) // many
    lax.fori_loop(0, whole, step, 0)
    if (hi - lo) % many:
        group(lo + whole * many, (hi - lo) % many)


def half(dst, src, t, coef, par, color, zs, lo, hi, ghosts=None, less=0.0):
    def f(i):
        c = at(src, i)
        rho = 1.0 / 6.0 if coef is None else coef[6, number(i)]
        new = c + (jacobian(src, i, zs, coef) - (at(t, i) - less)) * rho
        return [(dst, i, jnp.where(par == ((i + color) & 1), new, c))]

    planes(lo, hi, par.shape[0], f)
    if ghosts:
        ghosts(dst)


def pair_z(s, zs):
    even = (iota(s.shape, 1) // zs) & 1 == 0
    return s + jnp.where(even, roll(s, -zs, 1), roll(s, zs, 1))


def restrict(plane, i, zs, rows, slot, row0, n):
    s = pair_z(plane(i) + plane(i + 1), zs)
    slot = jnp.int32(number(slot))
    rows[slot, pl.ds(0, s.shape[0]), :] = s
    return rows[slot, pl.ds(row0, n, stride=2), :] + rows[slot, pl.ds(row0 + 1, n, stride=2), :]


def double_rows(x, rows, slot):
    n = x.shape[0]
    slot = jnp.int32(number(slot))
    rows[slot, pl.ds(0, n, stride=2), :] = x
    rows[slot, pl.ds(1, n, stride=2), :] = x


def down0(m, inv, u, d, msg, v, t, coef, va, rows):
    w = BLOCK + 2 * m
    cut = MARGINS[0] - m
    flat = coef is None
    par = parity(w, 1)

    def first(i):
        if flat:
            return [(va, i, jnp.where(par == (i & 1), at(d, i) * (-1.0 / 6.0), 0.0))]
        target = d[number(i + cut), cut : cut + w, :] * inv[0:1, :] - 1.0
        parts = hessian(u, i, 1)
        xx, yy, zz, xy, xz, yz = parts
        rho, stores = coef_of(coef, i, parts, 1.0)
        cubic = xx * yy + xx * zz + yy * zz - 0.0625 * (xy * xy + xz * xz + yz * yz)
        target = target - (xx + yy + zz) - 0.2 * cubic
        red = jnp.where(par == (i & 1), -target * rho, 0.0)
        return stores + [(t, i, target), (va, i, red)]

    edge = 0 if flat else 1
    planes(edge, w - edge, w, first)
    half(v, va, t, coef, par, 1, 1, edge + 1, w - edge - 1)
    lane_even = iota((8, LANES), 1) & 1 == 0

    def last(a):
        i = m + 2 * a
        t1 = 0.5 * restrict(lambda k: at(t, k) - jacobian(v, k, 1, coef), i, 1, rows, 2 * a, m, 8)
        if flat:
            u1 = jnp.zeros_like(t1)
        else:
            u1 = 0.125 * restrict(lambda k: at(u, k), i, 1, rows, 2 * a + 1, m, 8)
        return [(msg, a, jnp.where(lane_even, t1, u1))]

    planes(0, 8, 64, last)


def merged(*tables):
    out = tables[0]
    for x in tables[1:]:
        out = jnp.maximum(out, x)
    return out


def pack_density(density, own, lo, hi, known):
    m = MARGINS[0]
    half_block = BLOCK // 2
    total = jnp.sum(jnp.sum(density[...], axis=0), keepdims=True)
    for k in range(BLOCK):
        p = k if k < half_block else k + 2
        x = density[k]
        own[p] = x
        lo[p] = x[0:m]
        hi[p] = x[BLOCK - m : BLOCK]
    row = iota((BLOCK, LANES), 0)
    lane = iota((BLOCK, LANES), 1)
    for k in range(2):
        here = (row + 8 * k == lax.axis_index("gx")) & (lane == lax.axis_index("gy")) & (row < 8)
        table = jnp.where(here, total, 0.0)
        own[half_block + k] = table
        known[k] = table[0:8]
        lo[half_block + k] = table[0:m]
        hi[half_block + k] = table[0:m]


def join(before, own, after, far, out):
    m, half_block = MARGINS[0], BLOCK // 2
    for k in range(BLOCK + 2):
        out[k, 0:m, :] = before[k]
        out[k, m : m + BLOCK, :] = own[k]
        out[k, m + BLOCK :, :] = after[k]
    for k in range(2):
        out[half_block + k, m + 8 : m + 16, :] = far[k]


def start(m, db, do, da, far, msg, d, v, va, rows):
    half_block = BLOCK // 2
    for k in range(BLOCK):
        d[k + m] = do[k if k < half_block else k + 2]
    skip = BLOCK - m
    for k in range(m):
        d[k] = db[k if k + skip < half_block else k + 2]
        d[k + m + BLOCK] = da[k if k < half_block else k + 2]
    down0(m, None, None, d, msg, v, d, None, va, rows)
    for k in range(2):
        tables = []
        for ref, first in ((db, half_block - skip), (do, half_block), (da, half_block), (far, 0)):
            for row in (0, m, m + 8, m + BLOCK):
                tables.append(ref[first + k, row : row + 8, :])
        msg[8 + k] = merged(*tables)


def down1(turn, *refs):
    flat, lean = turn == 0, turn == len(MARGINS) - 1
    wb, wo, wa, msg, lo, hi, v, t = refs[:8]
    coef = u2 = None
    if flat:
        va, rows = refs[8:]
    elif lean:
        coef, va, u1, rows = refs[8:]
    else:
        coef, va, u1, u2, rows = refs[8:]
    par = parity(W1, 2)
    even = iota((W1, LANES), 1) & 1 == 0

    def unpack(a):
        stores = []
        for k, w in enumerate((wb, wo, wa)):
            i = a + 8 * k
            p = at(w, a)
            target = jnp.where(even, p, roll(p, 1, 1))
            stores.append((t, i, target))
            if flat:
                stores.append((va, i, jnp.where(par == (i & 1), target * (-1.0 / 6.0), 0.0)))
            else:
                stores.append((u1, i, jnp.where(even, roll(p, -1, 1), p)))
        return stores

    planes(0, 8, 40, unpack)
    if not flat:

        def first(i):
            rho, stores = coef_of(coef, i, hessian(u1, i, 2), 0.25)
            return stores + [(va, i, jnp.where(par == (i & 1), -at(t, i) * rho, 0.0))]

        planes(1, W1 - 1, W1, first)

    if u2 is not None:

        def coarse(a):
            u = 0.125 * restrict(lambda k: at(u1, k), 2 * a, 2, rows, a, 0, 12)
            return [(u2, (a, slice(0, 12)), u)]

        planes(0, 12, W1, coarse)
    half(v, va, t, coef, par, 1, 2, 1 if flat else 3, W1 - (1 if flat else 3))
    phase = iota((8, LANES), 1) & 3
    par2 = parity(8, 4)

    def last(a):
        t2 = 0.5 * restrict(lambda k: at(t, k) - jacobian(v, k, 2, coef), 4 + 2 * a, 2, rows, 2 * a, 4, 8)
        if flat:
            return [(msg, a, t2)]
        if lean:
            u = 0.125 * restrict(lambda k: at(u1, k), 4 + 2 * a, 2, rows, 2 * a + 1, 4, 8)
            return [(msg, a, jnp.where(phase == 1, u, t2))]
        xx, yy, zz = pures(u2, a + 2, 4)
        rho = relax_of(xx, yy, zz, 0.0625)
        slot = number(2 * a + 1)
        rows[slot, pl.ds(0, 16), :] = rho
        red = jnp.where(par2 == (a & 1), -t2 * rows[slot, pl.ds(2, 8), :], 0.0)
        uc = u2[number(a + 2), 2:10, :]
        return [(msg, a, jnp.where(phase == 1, uc, jnp.where(phase == 2, red, t2)))]

    planes(0, 8, 32, last)
    lo[0:4] = msg[0:4]
    hi[0:4] = msg[4:8]
    if flat:
        for k in range(2):
            table = merged(*[w[8 + k, 8 * j : 8 * j + 8, :] for w in (wb, wo, wa) for j in range(3)])
            msg[8 + k] = table
            lo[4 + k] = table
            hi[4 + k] = table


def repack(turn, w0, w1, w2, w3, w4, out, lo, hi):
    if turn == 0:
        for k in range(2):
            table = merged(*[w[w.shape[0] - 2 + k] for w in (w0, w1, w2, w3, w4)])
            out[8 + k] = table
            for ref in (lo, hi):
                ref[8 + 2 * k] = table[0:4]
                ref[9 + 2 * k] = table[4:8]
    phase = iota((8, LANES), 1) & 3
    where_from = [(w0, k) for k in range(4)]
    for w in (w1, w2, w3):
        where_from += [(w, k) for k in range(8)]
    where_from += [(w4, k) for k in range(4)]
    for a in range(CHUNK):
        for field in range(FIELDS[turn]):
            got = None
            for c in range(4):
                ref, k = where_from[a + CHUNK * c]
                part = ref[k]
                part = roll(part, c - field, 1) if c != field else part
                got = part if got is None else jnp.where(phase == c, part, got)
            out[CHUNK * field + a] = got
            lo[CHUNK * field + a] = got[0:4]
            hi[CHUNK * field + a] = got[4:8]


def ghosts_of(n):
    def fill(v):
        v[0] = roll(v[n], 1, 1)
        v[n + 1] = roll(v[1], -1, 1)

    return fill


def spread(x, c):
    phase = iota(x.shape, 1) & 3
    x = jnp.where(phase == c, x, 0.0)
    x = x + roll(x, -1 if c & 1 else 1, 1)
    return x + roll(x, -2 if c & 2 else 2, 1)


def mean_of(w2, cells):
    total = None
    for k in range(2):
        for h in range(2):
            tables = [w[8 + k, 4 * h : 4 * h + 4, :] for w in w2[1:4]]
            part = merged(*tables, w2[0][8 + 2 * k + h], w2[4][8 + 2 * k + h])
            total = part if total is None else total + part
    return jnp.sum(total, keepdims=True) * (1.0 / cells)


def up(m, turn, w2, s1, s0, u, mean, out, scratch):
    flat = turn == 0
    v1, t1, c1 = s1
    v0, t0, c0 = s0
    u2, t2, va, vb, c2, u3, t3, e3, f3, c3, rows, v1b, v1c, v0b, v0c = scratch
    n2, n3 = CHUNK, CHUNK // 2
    g2, g3 = ghosts_of(n2), ghosts_of(n3)
    par2, par3 = parity(W2, 4), parity(W2 // 2, 8)

    def load(a):
        for field, ref in enumerate((t2, u2, va)[: FIELDS[turn]]):
            row = 0
            for piece in w2:
                n = piece.shape[1]
                x = piece[CHUNK * field + a]
                ref[a + 1, row : row + n, :] = x - 16.0 * mean if flat else x
                row += n
        if flat:
            va[a + 1] = jnp.where(par2 == (a & 1), t2[a + 1] * (-1.0 / 6.0), 0.0)

    for a in range(n2):
        load(a)
    if flat:
        c2 = c3 = None
    else:
        g2(u2)

        def first2(i):
            rho, stores = coef_of(c2, i, hessian(u2, i, 4), 0.0625)
            if FIELDS[turn] == 2:
                stores.append((va, i, jnp.where(par2 == ((i + 1) & 1), -at(t2, i) * rho, 0.0)))
            return stores

        planes(1, n2 + 1, W2, first2)
    g2(va)
    half(vb, va, t2, c2, par2, 0, 4, 1, n2 + 1, g2)
    less0 = less1 = 0.0
    if flat:
        less0, less1 = mean, 4.0 * mean

    def first_sweep(par, scale, i):
        if not flat:
            return 0.0
        return jnp.where(par == (i & 1), (scale / 6.0) * mean, (scale / 3.0) * mean)

    def coarse(a):
        t = 0.5 * restrict(lambda k: at(t2, k) - jacobian(vb, k, 4, c2), 2 * a + 1, 4, rows, 2 * a, 0, 16)
        stores = [(t3, a + 1, t)]
        if not flat:
            x = 0.125 * restrict(lambda k: at(u2, k), 2 * a + 1, 4, rows, 2 * a + 1, 0, 16)
            stores.append((u3, a + 1, x))
        return stores

    planes(0, n3, 40, coarse)
    if not flat:
        g3(u3)

    def first(i):
        rho, stores = 1.0 / 6.0, []
        if not flat:
            rho, stores = coef_of(c3, i, hessian(u3, i, 8), 0.015625)
        return stores + [(e3, i, jnp.where(par3 == ((i + 1) & 1), -at(t3, i) * rho, 0.0))]

    planes(1, n3 + 1, W2 // 2, first)
    g3(e3)
    half(f3, e3, t3, c3, par3, 0, 8, 1, n3 + 1, g3)
    half(e3, f3, t3, c3, par3, 1, 8, 1, n3 + 1, g3)
    half(f3, e3, t3, c3, par3, 0, 8, 1, n3 + 1)

    for a in range(n3):
        double_rows(f3[a + 1], rows, a)
        e = rows[a, pl.ds(0, W2), :]
        va[2 * a + 1] = vb[2 * a + 1] + e
        va[2 * a + 2] = vb[2 * a + 2] + e
    g2(va)
    half(vb, va, t2, c2, par2, 1, 4, 1, n2 + 1, g2)
    half(va, vb, t2, c2, par2, 0, 4, 1, n2 + 1)

    par1 = parity(W1, 2)
    par0 = parity(BLOCK + 2 * m, 1)
    for x in range(W1 // 2):
        k = x + 10
        double_rows(spread(va[(k & 7) + 1], k >> 3), rows, x)
        e = rows[x, pl.ds(20, W1), :]
        v1b[2 * x] = v1[2 * x] + (e + first_sweep(par1, 4.0, 0))
        v1b[2 * x + 1] = v1[2 * x + 1] + (e + first_sweep(par1, 4.0, 1))
    r1 = m // 2
    half(v1c, v1b, t1, c1, par1, 0, 2, 8 - r1, 16 + r1, None, less1)
    half(v1b, v1c, t1, c1, par1, 1, 2, 9 - r1, 15 + r1, None, less1)

    w = BLOCK + 2 * m

    def raise0(a):
        double_rows(at(v1b, 8 - m // 2 + a), rows, a)
        e = rows[number(a), pl.ds(16 - m, w), :]
        return [
            (v0b, 2 * a + k, at(v0, 2 * a + k) + (e + first_sweep(par0, 1.0, k))) for k in range(2)
        ]

    planes(1, w // 2 - 1, w, raise0)
    half(v0c, v0b, t0, c0, par0, 0, 1, 3, w - 3, None, less0)
    inv = 1.0 / mean if flat else None

    def final(a):
        i = a + 4
        c = at(v0c, i)
        rho = 1.0 / 6.0 if flat else c0[6, number(i)]
        new = c + (jacobian(v0c, i, 1, c0) - (at(t0, i) - less0)) * rho
        new = jnp.where(par0 == ((i + 1) & 1), new, c)
        new = new * inv if flat else new + at(u, i)
        return [(out, a, new[4 : w - 4])]

    planes(0, w - 8, w, final)


def turn_end(m, cells, turn, *refs):
    refs = list(refs)

    def take(n):
        got = refs[:n]
        del refs[:n]
        return got

    flat, ends = turn == 0, turn == len(MARGINS) - 1
    w2 = take(5)
    if flat:
        d, v1, t1, v0 = take(4)
        s1, s0, u = (v1, t1, None), (v0, d, None), None
    else:
        inv, d = (None, None) if ends else take(2)
        s1, s0, (u,) = take(3), take(3), take(1)
    (out,) = take(1)
    mean = None
    if flat:
        (inv,) = take(1)
        mean = mean_of(w2, cells)
        inv[...] = jnp.broadcast_to(1.0 / mean, inv.shape)
    msg, v, t, coef = (None,) * 4 if ends else take(4)
    up(m, turn, w2, s1, s0, u, mean, out, refs[:15])
    if not ends:
        down0(m - 4, inv, out, d, msg, v, t, coef, refs[15], refs[10])


def f32(*shape):
    return jax.ShapeDtypeStruct(shape, jnp.float32)


def scr(*shape):
    return pltpu.VMEM(shape, jnp.float32)


def call(body, name, outs, scratch, args):
    specs = [pl.BlockSpec(memory_space=VMEM)] * len(args)
    return pl.pallas_call(
        body,
        out_shape=outs,
        in_specs=specs,
        out_specs=[pl.BlockSpec(memory_space=VMEM)] * len(outs),
        scratch_shapes=scratch,
        interpret=INTERPRET,
        compiler_params=pltpu.CompilerParams(vmem_limit_bytes=16 << 20),
        name=name,
    )(*args)


def shift(x, axis, by):
    n = lax.axis_size(axis)
    return lax.ppermute(x, axis, [((i + by) % n, i) for i in range(n)])


def neighbours(x, axis, dim, width):
    n = x.shape[dim]
    before = shift(lax.slice_in_dim(x, n - width, n, axis=dim), axis, -1)
    after = shift(lax.slice_in_dim(x, 0, width, axis=dim), axis, 1)
    return before, x, after


def wide(x, lo, hi, axis):
    if axis == "gx":
        ends = shift(lo, axis, -3), shift(hi, axis, 3)
    else:
        ends = shift(hi, axis, -4), shift(lo, axis, 4)
    return ends[0], shift(x, axis, -2), x, shift(x, axis, 2), ends[1]


def per_device(density):
    cells = float(density.size * lax.axis_size("gx") * lax.axis_size("gy"))
    m = MARGINS[0]
    w = BLOCK + 2 * m
    n = BLOCK + 2
    outs = [f32(n, BLOCK, LANES), f32(n, m, LANES), f32(n, m, LANES), f32(2, 8, LANES)]
    own, lo, hi, known = call(pack_density, "pack", outs, [], [density])
    args = [shift(hi, "gy", -1), own, shift(lo, "gy", 1), shift(known, "gy", 4)]
    (d,) = call(join, "join", [f32(n, w, LANES)], [], args)
    far = shift(d[BLOCK // 2 : BLOCK // 2 + 2], "gx", 6)
    rows = scr(24, 64, LANES)
    msg, d, v0 = call(
        functools.partial(start, m),
        "start",
        [f32(10, 8, LANES)] + [f32(w, w, LANES)] * 2,
        [scr(w, w, LANES), rows],
        [*neighbours(d, "gx", 0, m + 2), far],
    )
    for turn, m in enumerate(MARGINS):
        flat, ends = turn == 0, turn == len(MARGINS) - 1
        w = BLOCK + 2 * m
        extra = 2 if flat else 0
        w1 = jnp.concatenate(neighbours(msg, "gy", 1, 8), 1)
        outs = [f32(8 + extra, 8, LANES)] + [f32(4 + extra, 8, LANES)] * 2
        outs += [f32(W1, W1, LANES)] * 2
        scratch = [scr(W1, W1, LANES)]
        if not flat:
            outs.append(f32(7, W1, W1, LANES))
            scratch += [scr(W1, W1, LANES)] + ([] if ends else [scr(12, 16, LANES)])
        msg, lo, hi, *s1 = call(
            functools.partial(down1, turn),
            f"down1_{turn}",
            outs,
            scratch + [rows],
            neighbours(w1, "gx", 0, w1.shape[0]),
        )
        size = CHUNK * FIELDS[turn]
        outs = [f32(size + extra, 8, LANES)] + [f32(size + 2 * extra, 4, LANES)] * 2
        got = call(functools.partial(repack, turn), f"repack_{turn}", outs, [], wide(msg, lo, hi, "gx"))
        args = list(wide(*got, "gy"))
        if flat:
            args += [d, *s1, v0]
        else:
            args += ([] if ends else [inv, d]) + [*s1, *s0, u]
        a2 = scr(CHUNK + 2, W2, LANES)
        a3 = scr(CHUNK // 2 + 2, W2 // 2, LANES)
        scratch = [a2, a2, a2, a2, scr(7, CHUNK + 2, W2, LANES)]
        scratch += [a3, a3, a3, a3, scr(7, CHUNK // 2 + 2, W2 // 2, LANES)]
        scratch += [rows] + [scr(W1, W1, LANES)] * 2 + [scr(w, w, LANES)] * 2
        n = w - 8
        outs = [f32(n, n, LANES)] + ([f32(8, LANES)] if flat else [])
        if not ends:
            outs += [f32(8, 8, LANES), f32(n, n, LANES), f32(n, n, LANES), f32(7, n, n, LANES)]
            scratch += [scr(n, n, LANES)]
        u, *got = call(functools.partial(turn_end, m, cells, turn), f"up_{turn}", outs, scratch, args)
        if flat:
            inv, *got = got
        if not ends:
            msg, *s0 = got
    return u


def solution(mesh):
    spec = P("gx", "gy", None)
    return jax.shard_map(per_device, mesh=mesh, in_specs=(spec,), out_specs=spec, check_vma=False)
```

```python
import functools

import jax
import jax.numpy as jnp
from jax import lax
from jax.experimental import pallas as pl
from jax.experimental.pallas import tpu as pltpu
from jax.sharding import PartitionSpec as P


INTERPRET = False
LANES = 128
BLOCK = 16
MARGINS = (12, 8, 4)
FIELDS = (1, 3, 2)
W1 = 24
W2 = 32
CHUNK = 8
VMEM = pltpu.MemorySpace.VMEM
SMEM = pltpu.MemorySpace.SMEM
GROUP = 32


def roll(x, shift, axis):
    return pltpu.roll(x, shift % x.shape[axis], axis)


def iota(shape, axis):
    return lax.broadcasted_iota(jnp.int32, shape, axis)


def parity(rows, zs):
    shape = (rows, LANES)
    return (iota(shape, 0) + iota(shape, 1) // zs) & 1


class Place:
    def __init__(self, base, scale=1, offset=0):
        self.base, self.scale, self.offset = base, scale, offset

    def __add__(self, n):
        return Place(self.base, self.scale, self.offset + n)

    __radd__ = __add__

    def __sub__(self, n):
        return self + (-n)

    def __mul__(self, n):
        return Place(self.base, self.scale * n, self.offset * n)

    __rmul__ = __mul__

    def __and__(self, n):
        return self.value() & n

    def value(self):
        return self.base * self.scale + self.offset


SHARED = {}


def number(i):
    return i.value() if isinstance(i, Place) else i


def shared(kind, v, i, make):
    if not isinstance(i, Place):
        return make()
    key = (kind, id(v), i.scale, i.offset)
    if key not in SHARED:
        SHARED[key] = make()
    return SHARED[key]


def at(v, i):
    return shared("plane", v, i, lambda: v[number(i)])


def across(v, i, step, axis):
    def make():
        c = at(v, i)
        after, before = roll(c, -step, axis), roll(c, step, axis)
        return after + before, after - before

    return shared(axis, v, i, make)


def pures(v, i, zs):
    c2 = 2.0 * at(v, i)
    xx = at(v, i + 1) + at(v, i - 1) - c2
    return xx, across(v, i, 1, 0)[0] - c2, across(v, i, zs, 1)[0] - c2


def hessian(v, i, zs):
    xx, yy, zz = pures(v, i, zs)
    xy = across(v, i + 1, 1, 0)[1] - across(v, i - 1, 1, 0)[1]
    xz = across(v, i + 1, zs, 1)[1] - across(v, i - 1, zs, 1)[1]
    dz = across(v, i, zs, 1)[1]
    yz = roll(dz, -1, 0) - roll(dz, 1, 0)
    return xx, yy, zz, xy, xz, yz


def jacobian(v, i, zs, coef):
    if coef is None:
        around = across(v, i, 1, 0)[0] + across(v, i, zs, 1)[0]
        return at(v, i + 1) + at(v, i - 1) + around - 6.0 * at(v, i)
    parts = hessian(v, i, zs)
    k = number(i)
    out = coef[0, k] * parts[0]
    for n in range(1, 6):
        out = out + coef[n, k] * parts[n]
    return out


def coef_of(coef, i, parts, s):
    xx, yy, zz, xy, xz, yz = parts
    g = 0.2 * s
    h = -0.025 * s
    rho = relax_of(xx, yy, zz, s)
    values = (1.0 + g * (yy + zz), 1.0 + g * (xx + zz), 1.0 + g * (xx + yy), h * xy, h * xz, h * yz, rho)
    return rho, [(coef, (n, i), value) for n, value in enumerate(values)]


def relax_of(xx, yy, zz, s):
    return 1.0 / jnp.maximum(6.0 + (0.8 * s) * (xx + yy + zz), 3.0)


def loop(lo, hi, f):
    def step(i, carry):
        f(i)
        return carry

    lax.fori_loop(lo, hi, step, 0)


def group_size(count, most):
    if count <= most:
        return count
    best = max(k for k in range(1, most + 1) if count % k == 0)
    return best if 2 * best > most else most


def planes(lo, hi, rows, f):
    many = group_size(hi - lo, GROUP // (rows // 8))

    def group(first, count):
        SHARED.clear()
        done = [f(Place(first) + k) for k in range(count)]
        SHARED.clear()
        for stores in done:
            for ref, i, value in stores:
                ref[tuple(map(number, i)) if isinstance(i, tuple) else number(i)] = value

    def step(g, carry):
        group(lo + g * many, many)
        return carry

    whole = (hi - lo) // many
    lax.fori_loop(0, whole, step, 0)
    if (hi - lo) % many:
        group(lo + whole * many, (hi - lo) % many)


def half(dst, src, t, coef, par, color, zs, lo, hi, ghosts=None, less=0.0):
    def f(i):
        c = at(src, i)
        rho = 1.0 / 6.0 if coef is None else coef[6, number(i)]
        new = c + (jacobian(src, i, zs, coef) - (at(t, i) - less)) * rho
        return [(dst, i, jnp.where(par == ((i + color) & 1), new, c))]

    planes(lo, hi, par.shape[0], f)
    if ghosts:
        ghosts(dst)


def pair_z(s, zs):
    even = (iota(s.shape, 1) // zs) & 1 == 0
    return s + jnp.where(even, roll(s, -zs, 1), roll(s, zs, 1))


def restrict(plane, i, zs, rows, slot, row0, n):
    s = pair_z(plane(i) + plane(i + 1), zs)
    slot = jnp.int32(number(slot))
    rows[slot, pl.ds(0, s.shape[0]), :] = s
    return rows[slot, pl.ds(row0, n, stride=2), :] + rows[slot, pl.ds(row0 + 1, n, stride=2), :]


def double_rows(x, rows, slot):
    n = x.shape[0]
    slot = jnp.int32(number(slot))
    rows[slot, pl.ds(0, n, stride=2), :] = x
    rows[slot, pl.ds(1, n, stride=2), :] = x


def down0(m, inv, u, d, msg, v, t, coef, va, rows):
    w = BLOCK + 2 * m
    cut = MARGINS[0] - m
    flat = coef is None
    par = parity(w, 1)

    def first(i):
        if flat:
            return [(va, i, jnp.where(par == (i & 1), at(d, i) * (-1.0 / 6.0), 0.0))]
        target = d[number(i + cut), cut : cut + w, :] * inv[0:1, :] - 1.0
        parts = hessian(u, i, 1)
        xx, yy, zz, xy, xz, yz = parts
        rho, stores = coef_of(coef, i, parts, 1.0)
        cubic = xx * yy + xx * zz + yy * zz - 0.0625 * (xy * xy + xz * xz + yz * yz)
        target = target - (xx + yy + zz) - 0.2 * cubic
        red = jnp.where(par == (i & 1), -target * rho, 0.0)
        return stores + [(t, i, target), (va, i, red)]

    edge = 0 if flat else 1
    planes(edge, w - edge, w, first)
    half(v, va, t, coef, par, 1, 1, edge + 1, w - edge - 1)
    lane_even = iota((8, LANES), 1) & 1 == 0

    def last(a):
        i = m + 2 * a
        t1 = 0.5 * restrict(lambda k: at(t, k) - jacobian(v, k, 1, coef), i, 1, rows, 2 * a, m, 8)
        if flat:
            u1 = jnp.zeros_like(t1)
        else:
            u1 = 0.125 * restrict(lambda k: at(u, k), i, 1, rows, 2 * a + 1, m, 8)
        return [(msg, a, jnp.where(lane_even, t1, u1))]

    planes(0, 8, 64, last)


def merged(*tables):
    out = tables[0]
    for x in tables[1:]:
        out = jnp.maximum(out, x)
    return out


def pack_density(density, own, lo, hi, known):
    m = MARGINS[0]
    half_block = BLOCK // 2
    total = jnp.sum(jnp.sum(density[...], axis=0), keepdims=True)
    for k in range(BLOCK):
        p = k if k < half_block else k + 2
        x = density[k]
        own[p] = x
        lo[p] = x[0:m]
        hi[p] = x[BLOCK - m : BLOCK]
    row = iota((BLOCK, LANES), 0)
    lane = iota((BLOCK, LANES), 1)
    for k in range(2):
        here = (row + 8 * k == lax.axis_index("gx")) & (lane == lax.axis_index("gy")) & (row < 8)
        table = jnp.where(here, total, 0.0)
        own[half_block + k] = table
        known[k] = table[0:8]
        lo[half_block + k] = table[0:m]
        hi[half_block + k] = table[0:m]


def join(before, own, after, far, out):
    m, half_block = MARGINS[0], BLOCK // 2
    for k in range(BLOCK + 2):
        out[k, 0:m, :] = before[k]
        out[k, m : m + BLOCK, :] = own[k]
        out[k, m + BLOCK :, :] = after[k]
    for k in range(2):
        out[half_block + k, m + 8 : m + 16, :] = far[k]


def start(m, db, do, da, far, msg, d, v, va, rows):
    half_block = BLOCK // 2
    for k in range(BLOCK):
        d[k + m] = do[k if k < half_block else k + 2]
    skip = BLOCK - m
    for k in range(m):
        d[k] = db[k if k + skip < half_block else k + 2]
        d[k + m + BLOCK] = da[k if k < half_block else k + 2]
    down0(m, None, None, d, msg, v, d, None, va, rows)
    for k in range(2):
        tables = []
        for ref, first in ((db, half_block - skip), (do, half_block), (da, half_block), (far, 0)):
            for row in (0, m, m + 8, m + BLOCK):
                tables.append(ref[first + k, row : row + 8, :])
        msg[8 + k] = merged(*tables)


def down1(turn, *refs):
    flat, lean = turn == 0, turn == len(MARGINS) - 1
    wb, wo, wa, msg, lo, hi, v, t = refs[:8]
    coef = u2 = None
    if flat:
        va, rows = refs[8:]
    elif lean:
        coef, va, u1, rows = refs[8:]
    else:
        coef, va, u1, u2, rows = refs[8:]
    par = parity(W1, 2)
    even = iota((W1, LANES), 1) & 1 == 0

    def unpack(a):
        stores = []
        for k, w in enumerate((wb, wo, wa)):
            i = a + 8 * k
            p = at(w, a)
            target = jnp.where(even, p, roll(p, 1, 1))
            stores.append((t, i, target))
            if flat:
                stores.append((va, i, jnp.where(par == (i & 1), target * (-1.0 / 6.0), 0.0)))
            else:
                stores.append((u1, i, jnp.where(even, roll(p, -1, 1), p)))
        return stores

    planes(0, 8, 40, unpack)
    if not flat:

        def first(i):
            rho, stores = coef_of(coef, i, hessian(u1, i, 2), 0.25)
            return stores + [(va, i, jnp.where(par == (i & 1), -at(t, i) * rho, 0.0))]

        planes(1, W1 - 1, W1, first)

    if u2 is not None:

        def coarse(a):
            u = 0.125 * restrict(lambda k: at(u1, k), 2 * a, 2, rows, a, 0, 12)
            return [(u2, (a, slice(0, 12)), u)]

        planes(0, 12, W1, coarse)
    half(v, va, t, coef, par, 1, 2, 1 if flat else 3, W1 - (1 if flat else 3))
    phase = iota((8, LANES), 1) & 3
    par2 = parity(8, 4)

    def last(a):
        t2 = 0.5 * restrict(lambda k: at(t, k) - jacobian(v, k, 2, coef), 4 + 2 * a, 2, rows, 2 * a, 4, 8)
        if flat:
            return [(msg, a, t2)]
        if lean:
            u = 0.125 * restrict(lambda k: at(u1, k), 4 + 2 * a, 2, rows, 2 * a + 1, 4, 8)
            return [(msg, a, jnp.where(phase == 1, u, t2))]
        xx, yy, zz = pures(u2, a + 2, 4)
        rho = relax_of(xx, yy, zz, 0.0625)
        slot = number(2 * a + 1)
        rows[slot, pl.ds(0, 16), :] = rho
        red = jnp.where(par2 == (a & 1), -t2 * rows[slot, pl.ds(2, 8), :], 0.0)
        uc = u2[number(a + 2), 2:10, :]
        return [(msg, a, jnp.where(phase == 1, uc, jnp.where(phase == 2, red, t2)))]

    planes(0, 8, 32, last)
    lo[0:4] = msg[0:4]
    hi[0:4] = msg[4:8]
    if flat:
        for k in range(2):
            table = merged(*[w[8 + k, 8 * j : 8 * j + 8, :] for w in (wb, wo, wa) for j in range(3)])
            msg[8 + k] = table
            lo[4 + k] = table
            hi[4 + k] = table


def repack(turn, w0, w1, w2, w3, w4, out, lo, hi):
    if turn == 0:
        for k in range(2):
            table = merged(*[w[w.shape[0] - 2 + k] for w in (w0, w1, w2, w3, w4)])
            out[8 + k] = table
            for ref in (lo, hi):
                ref[8 + 2 * k] = table[0:4]
                ref[9 + 2 * k] = table[4:8]
    phase = iota((8, LANES), 1) & 3
    where_from = [(w0, k) for k in range(4)]
    for w in (w1, w2, w3):
        where_from += [(w, k) for k in range(8)]
    where_from += [(w4, k) for k in range(4)]
    for a in range(CHUNK):
        for field in range(FIELDS[turn]):
            got = None
            for c in range(4):
                ref, k = where_from[a + CHUNK * c]
                part = ref[k]
                part = roll(part, c - field, 1) if c != field else part
                got = part if got is None else jnp.where(phase == c, part, got)
            if field < 2:
                out[CHUNK * field + a] = got
            elif a in (0, CHUNK - 1):
                out[CHUNK * field + a // (CHUNK - 1)] = got
            lo[CHUNK * field + a] = got[0:4]
            hi[CHUNK * field + a] = got[4:8]


def ghosts_of(n):
    def fill(v):
        v[0] = roll(v[n], 1, 1)
        v[n + 1] = roll(v[1], -1, 1)

    return fill


def spread(x, c):
    phase = iota(x.shape, 1) & 3
    x = jnp.where(phase == c, x, 0.0)
    x = x + roll(x, -1 if c & 1 else 1, 1)
    return x + roll(x, -2 if c & 2 else 2, 1)


def mean_of(w2, cells):
    total = None
    for k in range(2):
        for h in range(2):
            tables = [w[8 + k, 4 * h : 4 * h + 4, :] for w in w2[1:4]]
            part = merged(*tables, w2[0][8 + 2 * k + h], w2[4][8 + 2 * k + h])
            total = part if total is None else total + part
    return jnp.sum(total, keepdims=True) * (1.0 / cells)


def up(m, turn, w2, s1, s0, u, mean, out, scratch):
    flat = turn == 0
    v1, t1, c1 = s1
    v0, t0, c0 = s0
    u2, t2, va, vb, c2, u3, t3, e3, f3, c3, rows, v1b, v1c, v0b, v0c = scratch
    n2, n3 = CHUNK, CHUNK // 2
    g2, g3 = ghosts_of(n2), ghosts_of(n3)
    par2, par3 = parity(W2, 4), parity(W2 // 2, 8)

    def load(a):
        for field, ref in enumerate((t2, u2, va)[: FIELDS[turn]]):
            row = 0
            for piece in w2:
                n = piece.shape[1]
                at_end = a in (0, CHUNK - 1)
                if field == 2 and n == 8 and not at_end:
                    row += n
                    continue
                x = piece[CHUNK * field + (a // (CHUNK - 1) if field == 2 and n == 8 else a)]
                ref[a + 1, row : row + n, :] = x - 16.0 * mean if flat else x
                row += n
        if flat:
            va[a + 1] = jnp.where(par2 == (a & 1), t2[a + 1] * (-1.0 / 6.0), 0.0)

    for a in range(n2):
        load(a)
    if flat:
        c2 = c3 = None
    else:
        g2(u2)

        row = iota((W2, LANES), 0)
        phase = iota((W2, LANES), 1) & 3
        edge_rows = (row == 0) | (row == W2 - 1)

        def first2(i):
            rho, stores = coef_of(c2, i, hessian(u2, i, 4), 0.0625)
            red = jnp.where(par2 == ((i + 1) & 1), -at(t2, i) * rho, 0.0)
            if FIELDS[turn] == 3:
                k = number(i)
                shell = edge_rows | ((phase == 0) & (k == 1)) | ((phase == 3) & (k == n2))
                red = jnp.where(shell, at(va, i), red)
            return stores + [(va, i, red)]

        planes(1, n2 + 1, W2, first2)
    g2(va)
    half(vb, va, t2, c2, par2, 0, 4, 1, n2 + 1, g2)
    less0 = less1 = 0.0
    if flat:
        less0, less1 = mean, 4.0 * mean

    def first_sweep(par, scale, i):
        if not flat:
            return 0.0
        return jnp.where(par == (i & 1), (scale / 6.0) * mean, (scale / 3.0) * mean)

    def coarse(a):
        t = 0.5 * restrict(lambda k: at(t2, k) - jacobian(vb, k, 4, c2), 2 * a + 1, 4, rows, 2 * a, 0, 16)
        stores = [(t3, a + 1, t)]
        if not flat:
            x = 0.125 * restrict(lambda k: at(u2, k), 2 * a + 1, 4, rows, 2 * a + 1, 0, 16)
            stores.append((u3, a + 1, x))
        return stores

    planes(0, n3, 40, coarse)
    if not flat:
        g3(u3)

    def first(i):
        rho, stores = 1.0 / 6.0, []
        if not flat:
            rho, stores = coef_of(c3, i, hessian(u3, i, 8), 0.015625)
        return stores + [(e3, i, jnp.where(par3 == ((i + 1) & 1), -at(t3, i) * rho, 0.0))]

    planes(1, n3 + 1, W2 // 2, first)
    g3(e3)
    half(f3, e3, t3, c3, par3, 0, 8, 1, n3 + 1, g3)
    half(e3, f3, t3, c3, par3, 1, 8, 1, n3 + 1, g3)
    half(f3, e3, t3, c3, par3, 0, 8, 1, n3 + 1)

    for a in range(n3):
        double_rows(f3[a + 1], rows, a)
        e = rows[a, pl.ds(0, W2), :]
        va[2 * a + 1] = vb[2 * a + 1] + e
        va[2 * a + 2] = vb[2 * a + 2] + e
    g2(va)
    half(vb, va, t2, c2, par2, 1, 4, 1, n2 + 1, g2)
    half(va, vb, t2, c2, par2, 0, 4, 1, n2 + 1)

    par1 = parity(W1, 2)
    par0 = parity(BLOCK + 2 * m, 1)
    for x in range(W1 // 2):
        k = x + 10
        double_rows(spread(va[(k & 7) + 1], k >> 3), rows, x)
        e = rows[x, pl.ds(20, W1), :]
        v1b[2 * x] = v1[2 * x] + (e + first_sweep(par1, 4.0, 0))
        v1b[2 * x + 1] = v1[2 * x + 1] + (e + first_sweep(par1, 4.0, 1))
    r1 = m // 2
    half(v1c, v1b, t1, c1, par1, 0, 2, 8 - r1, 16 + r1, None, less1)
    half(v1b, v1c, t1, c1, par1, 1, 2, 9 - r1, 15 + r1, None, less1)

    w = BLOCK + 2 * m

    def raise0(a):
        double_rows(at(v1b, 8 - m // 2 + a), rows, a)
        e = rows[number(a), pl.ds(16 - m, w), :]
        return [
            (v0b, 2 * a + k, at(v0, 2 * a + k) + (e + first_sweep(par0, 1.0, k))) for k in range(2)
        ]

    planes(1, w // 2 - 1, w, raise0)
    half(v0c, v0b, t0, c0, par0, 0, 1, 3, w - 3, None, less0)
    inv = 1.0 / mean if flat else None

    def final(a):
        i = a + 4
        c = at(v0c, i)
        rho = 1.0 / 6.0 if flat else c0[6, number(i)]
        new = c + (jacobian(v0c, i, 1, c0) - (at(t0, i) - less0)) * rho
        new = jnp.where(par0 == ((i + 1) & 1), new, c)
        new = new * inv if flat else new + at(u, i)
        return [(out, a, new[4 : w - 4])]

    planes(0, w - 8, w, final)


def turn_end(m, cells, turn, *refs):
    refs = list(refs)

    def take(n):
        got = refs[:n]
        del refs[:n]
        return got

    flat, ends = turn == 0, turn == len(MARGINS) - 1
    w2 = take(5)
    if flat:
        d, v1, t1, v0 = take(4)
        s1, s0, u = (v1, t1, None), (v0, d, None), None
    else:
        inv, d = (None, None) if ends else take(2)
        s1, s0, (u,) = take(3), take(3), take(1)
    (out,) = take(1)
    mean = None
    if flat:
        (inv,) = take(1)
        mean = mean_of(w2, cells)
        inv[...] = jnp.broadcast_to(1.0 / mean, inv.shape)
    msg, v, t, coef = (None,) * 4 if ends else take(4)
    up(m, turn, w2, s1, s0, u, mean, out, refs[:15])
    if not ends:
        down0(m - 4, inv, out, d, msg, v, t, coef, refs[15], refs[10])


def f32(*shape):
    return jax.ShapeDtypeStruct(shape, jnp.float32)


def scr(*shape):
    return pltpu.VMEM(shape, jnp.float32)


def call(body, name, outs, scratch, args):
    specs = [pl.BlockSpec(memory_space=VMEM)] * len(args)
    return pl.pallas_call(
        body,
        out_shape=outs,
        in_specs=specs,
        out_specs=[pl.BlockSpec(memory_space=VMEM)] * len(outs),
        scratch_shapes=scratch,
        interpret=INTERPRET,
        compiler_params=pltpu.CompilerParams(vmem_limit_bytes=16 << 20),
        name=name,
    )(*args)


def shift(x, axis, by):
    n = lax.axis_size(axis)
    return lax.ppermute(x, axis, [((i + by) % n, i) for i in range(n)])


def neighbours(x, axis, dim, width):
    n = x.shape[dim]
    before = shift(lax.slice_in_dim(x, n - width, n, axis=dim), axis, -1)
    after = shift(lax.slice_in_dim(x, 0, width, axis=dim), axis, 1)
    return before, x, after


def wide(x, lo, hi, axis):
    if axis == "gx":
        ends = shift(lo, axis, -3), shift(hi, axis, 3)
    else:
        ends = shift(hi, axis, -4), shift(lo, axis, 4)
    return ends[0], shift(x, axis, -2), x, shift(x, axis, 2), ends[1]


def per_device(density):
    cells = float(density.size * lax.axis_size("gx") * lax.axis_size("gy"))
    m = MARGINS[0]
    w = BLOCK + 2 * m
    n = BLOCK + 2
    outs = [f32(n, BLOCK, LANES), f32(n, m, LANES), f32(n, m, LANES), f32(2, 8, LANES)]
    own, lo, hi, known = call(pack_density, "pack", outs, [], [density])
    args = [shift(hi, "gy", -1), own, shift(lo, "gy", 1), shift(known, "gy", 4)]
    (d,) = call(join, "join", [f32(n, w, LANES)], [], args)
    far = shift(d[BLOCK // 2 : BLOCK // 2 + 2], "gx", 6)
    rows = scr(24, 64, LANES)
    msg, d, v0 = call(
        functools.partial(start, m),
        "start",
        [f32(10, 8, LANES)] + [f32(w, w, LANES)] * 2,
        [scr(w, w, LANES), rows],
        [*neighbours(d, "gx", 0, m + 2), far],
    )
    for turn, m in enumerate(MARGINS):
        flat, ends = turn == 0, turn == len(MARGINS) - 1
        w = BLOCK + 2 * m
        extra = 2 if flat else 0
        w1 = jnp.concatenate(neighbours(msg, "gy", 1, 8), 1)
        outs = [f32(8 + extra, 8, LANES)] + [f32(4 + extra, 8, LANES)] * 2
        outs += [f32(W1, W1, LANES)] * 2
        scratch = [scr(W1, W1, LANES)]
        if not flat:
            outs.append(f32(7, W1, W1, LANES))
            scratch += [scr(W1, W1, LANES)] + ([] if ends else [scr(12, 16, LANES)])
        msg, lo, hi, *s1 = call(
            functools.partial(down1, turn),
            f"down1_{turn}",
            outs,
            scratch + [rows],
            neighbours(w1, "gx", 0, w1.shape[0]),
        )
        size = CHUNK * FIELDS[turn]
        outs = [f32(min(size, 2 * CHUNK + 2) + extra, 8, LANES)] + [f32(size + 2 * extra, 4, LANES)] * 2
        got = call(functools.partial(repack, turn), f"repack_{turn}", outs, [], wide(msg, lo, hi, "gx"))
        args = list(wide(*got, "gy"))
        if flat:
            args += [d, *s1, v0]
        else:
            args += ([] if ends else [inv, d]) + [*s1, *s0, u]
        a2 = scr(CHUNK + 2, W2, LANES)
        a3 = scr(CHUNK // 2 + 2, W2 // 2, LANES)
        scratch = [a2, a2, a2, a2, scr(7, CHUNK + 2, W2, LANES)]
        scratch += [a3, a3, a3, a3, scr(7, CHUNK // 2 + 2, W2 // 2, LANES)]
        scratch += [rows] + [scr(W1, W1, LANES)] * 2 + [scr(w, w, LANES)] * 2
        n = w - 8
        outs = [f32(n, n, LANES)] + ([f32(8, LANES)] if flat else [])
        if not ends:
            outs += [f32(8, 8, LANES), f32(n, n, LANES), f32(n, n, LANES), f32(7, n, n, LANES)]
            scratch += [scr(n, n, LANES)]
        u, *got = call(functools.partial(turn_end, m, cells, turn), f"up_{turn}", outs, scratch, args)
        if flat:
            inv, *got = got
        if not ends:
            msg, *s0 = got
    return u


def solution(mesh):
    spec = P("gx", "gy", None)
    return jax.shard_map(per_device, mesh=mesh, in_specs=(spec,), out_specs=spec, check_vma=False)
```
